256 devices in a mesh: band: 16 (over y_lo, x, core), grid: 16 (over y_hi, z).
Axes of the slice: x: 4, y: 4 (y_hi: 2, y_lo: 2; y = y_hi * 2 + y_lo), z: 8, core: 2. Of those that a mesh axis runs over, the one named last changes fastest.
Arguments:
- orbitals: float32 [64, 48, 2304], P('band', 'grid'), may hold values from -5.5 to 6.6
- occupation: int32 [64], P('band'), may hold values from 0 to 2
- cutoff: int32 [], replicated, may hold values from 144 to 1728
Outputs:
- exchange_term: float32 [64, 48, 2304], P('band', 'grid')
The draws below stay inside these ranges and needn't reach their ends.
All inputs are finite; a program needn't handle non-finite values.
Results may differ from the reference program's by a relative error of at most 0.00005.
Values sent between devices are 32-bit elements; how exact they have to be, the bound alone decides.
No kernel may reach another device: no remote copies, remote signals or barrier semaphores. Data moves between devices by JAX's collectives and lax.ppermute only.
A program may use at most 128 MiB of HBM per device.

```python
import jax
import jax.numpy as jnp
from jax import lax

G = 48
M = 64


def draw_orbitals(key, part):
    rough = jnp.clip(jax.random.normal(key, (M, G, G * G), jnp.float32), -5.5, 5.5)
    return rough


def set_ends(values, rng, low, largest):
    longest = values.shape.index(max(values.shape))
    spots = []
    for shift in (0, 1):
        where = [jax.random.randint(jax.random.fold_in(rng, axis), (), 0, length) for axis, length in enumerate(values.shape)]
        where[longest] = (where[longest] + shift) % values.shape[longest]
        spots.append(tuple(where))
    return values.at[spots[0]].set(low).at[spots[1]].set(largest)


def setup_inputs(seed: int = 0) -> dict:
    splits = jax.random.split(jax.random.key(seed), 4)
    orbitals = draw_orbitals(jax.random.fold_in(splits[3], 71), 0)
    occupation = set_ends(jax.random.randint(splits[1], (M,), 0, 3), jax.random.fold_in(splits[1], 1), 0, 2).astype(jnp.int32)
    cutoff = jax.random.randint(splits[2], (), G * G // 16, 3 * (G // 2) * (G // 2) + 1).astype(jnp.int32)
    return dict(orbitals=orbitals, occupation=occupation, cutoff=cutoff)


screen_alpha = 2.0
screen_scale = 4.0


def reference(orbitals, occupation, cutoff):
    fields = orbitals.reshape(M, G, G, G)
    position = jnp.arange(G, dtype=jnp.int32)
    signed = jnp.where(position <= G // 2, position, position - G)
    shells = signed[:, None, None] ** 2 + signed[None, :, None] ** 2 + signed[None, None, :] ** 2
    ratios = shells.astype(jnp.float32) / screen_alpha
    screen = jnp.where(shells > 0, (1.0 - jnp.exp(-ratios)) / jnp.maximum(ratios, 1.0 / screen_alpha), 1.0)
    kernel = jnp.where(shells <= cutoff, screen_scale * screen, 0.0).astype(jnp.float32)
    weights = occupation.astype(jnp.float32) * 0.5

    def apply_row(orbital):
        densities = orbital[None] * fields
        spectrum = jnp.fft.fftn(densities, axes=(1, 2, 3)) * kernel[None]
        potential = jnp.real(jnp.fft.ifftn(spectrum, axes=(1, 2, 3)))
        return -jnp.sum(weights[:, None, None, None] * fields * potential, axis=0)

    return lax.map(apply_row, fields).reshape(M, G, G * G).astype(jnp.float32)
```

```python
import numpy as np
import jax
import jax.numpy as jnp
from jax import lax
from jax.experimental import pallas as pl
from jax.experimental.pallas import tpu as pltpu
from jax.sharding import PartitionSpec as P


G = 48
SLOTS = 10
WIDE = 512
YB = 8
LB = YB * G


def split2(x):
    hi = x.astype(jnp.bfloat16)
    lo = (x - hi.astype(jnp.float32)).astype(jnp.bfloat16)
    return jnp.concatenate([hi, lo], axis=0)


def apply(mat, x):
    both = jnp.dot(mat, split2(x), preferred_element_type=jnp.float32)
    return both[:G] + both[G:]


def kernel(idx, wts, own, vis, oth, ktab, fx, ix, fz, iz, home, back, spec, rows, cols, zed):
    gi = idx[0]
    gj = idx[1]

    def enter(yb, _):
        lanes = pl.ds(pl.multiple_of(yb * LB, LB), LB)
        v = [vis[0, :, lanes], vis[1, :, lanes]]
        for p in range(SLOTS):
            if p < 8:
                r = own[p % 4, :, lanes] * v[p // 4]
            elif p == 8:
                r = own[gi, :, lanes] * own[gj, :, lanes]
            else:
                r = own[gi, :, lanes] * oth[0, :, lanes]
            rows[p * G:(p + 1) * G, :] = apply(fx[...], r)
        for c in range(3):
            cols[c * 128:(c + 1) * 128, :] = rows[:, c * 128:(c + 1) * 128].T
        for y in range(YB):
            zed[y] = apply(fz[...], cols[y * G:(y + 1) * G, :])
        spec[:, pl.ds(pl.multiple_of(yb * YB, YB), YB), :] = jnp.swapaxes(zed[...], 0, 1)
        return 0

    lax.fori_loop(0, G // YB, enter, 0)

    def middle(k, _):
        for u in range(2):
            kz = k * 2 + u
            t = ktab[kz]
            t = jnp.concatenate([t, t[:, :WIDE - LB]], axis=1)
            s = apply(fz[...], spec[kz]) * t
            spec[kz] = apply(iz[...], s)
        return 0

    lax.fori_loop(0, G // 2, middle, 0)

    def leave(yb, _):
        lanes = pl.ds(pl.multiple_of(yb * LB, LB), LB)
        zed[...] = jnp.swapaxes(spec[:, pl.ds(pl.multiple_of(yb * YB, YB), YB), :], 0, 1)
        for y in range(YB):
            cols[y * G:(y + 1) * G, :] = apply(iz[...], zed[y])
        for c in range(3):
            rows[:, c * 128:(c + 1) * 128] = cols[c * 128:(c + 1) * 128, :].T
        b0 = None
        b1 = None
        v0 = vis[0, :, lanes] * wts[4]
        v1 = vis[1, :, lanes] * wts[5]
        for i in range(4):
            p0 = apply(ix[...], rows[i * G:(i + 1) * G, :])
            p1 = apply(ix[...], rows[(i + 4) * G:(i + 5) * G, :])
            home[i, :, lanes] = v0 * p0 + v1 * p1
            o = own[i, :, lanes] * wts[i]
            b0 = o * p0 if b0 is None else b0 + o * p0
            b1 = o * p1 if b1 is None else b1 + o * p1
        back[0, :, lanes] = b0
        back[1, :, lanes] = b1
        p8 = apply(ix[...], rows[8 * G:9 * G, :])
        p9 = apply(ix[...], rows[9 * G:10 * G, :])
        home[gi, :, lanes] = home[gi, :, lanes] + (own[gj, :, lanes] * wts[6]) * p8 + (oth[0, :, lanes] * wts[7]) * p9
        return 0

    lax.fori_loop(0, G // YB, leave, 0)


def pair_solver(idx, wts, own, vis, oth, ktab, fx, ix, fz, iz):
    vm = pl.BlockSpec(memory_space=pltpu.VMEM)
    sm = pl.BlockSpec(memory_space=pltpu.SMEM)
    return pl.pallas_call(
        kernel,
        out_shape=(jax.ShapeDtypeStruct((4, G, G * G), jnp.float32), jax.ShapeDtypeStruct((2, G, G * G), jnp.float32)),
        in_specs=[sm, sm] + [vm] * 8,
        out_specs=(vm, vm),
        scratch_shapes=[
            pltpu.VMEM((G, G, WIDE), jnp.float32),
            pltpu.VMEM((WIDE, LB), jnp.float32),
            pltpu.VMEM((LB, WIDE), jnp.float32),
            pltpu.VMEM((YB, G, WIDE), jnp.float32),
        ],
        compiler_params=pltpu.CompilerParams(vmem_limit_bytes=56 << 20),
        cost_estimate=pl.CostEstimate(flops=10**10, bytes_accessed=10**7, transcendentals=0),
    )(idx, wts, own, vis, oth, ktab, fx, ix, fz, iz)


def stacked(m):
    m = jnp.asarray(m, jnp.float32)
    top = lax.reduce_precision(m, 8, 7)
    hi = top.astype(jnp.bfloat16)
    lo = (m - top).astype(jnp.bfloat16)
    return jnp.concatenate([jnp.concatenate([hi, hi], 1), jnp.concatenate([lo, jnp.zeros_like(lo)], 1)], 0)


def basis(place):
    k = jnp.arange(G, dtype=jnp.int32)
    m = jnp.where(k <= G // 2, k, k - G // 2)
    ang = (2.0 * np.pi / G) * ((m[:, None] * place[None, :]) % G).astype(jnp.float32)
    return jnp.where((k <= G // 2)[:, None], jnp.cos(ang), jnp.sin(ang))


def kernel_table(cutoff):
    def freq(shape, dim, mod=None):
        k = lax.broadcasted_iota(jnp.int32, shape, dim)
        k = k % G if mod else k
        m = jnp.where(k <= G // 2, k, k - G // 2)
        return m * m, jnp.where((k == 0) | (k == G // 2), 1.0, 2.0)
    (a, wa), (b, wb), (c, wc) = freq((G, 1, 1), 0), freq((1, G, 1), 1), freq((1, 1, LB), 2, True)
    n = a + b + c
    ratios = n.astype(jnp.float32) * 0.5
    screen = jnp.where(n > 0, (1.0 - jnp.exp(-ratios)) / jnp.maximum(ratios, 0.5), 1.0)
    return jnp.where(n <= cutoff, 4.0 * screen * (wa * wb * wc / float(G**3)), 0.0)


def ring(block, axis, source):
    count = lax.axis_size(axis)
    return lax.ppermute(block, axis, [(source(i), i) for i in range(count)])


def partner(i):
    return (i + 8) % 16


def above(i):
    return i // 8 * 8 + (i + 1) % 8


def below(i):
    return i // 8 * 8 + (i + 7) % 8


def twin(i):
    return i ^ 1


def visit_route():
    bands, grids = lax.axis_size("band"), lax.axis_size("grid")
    pairs = []
    for b in range(bands):
        for g in range(grids):
            pairs.append(((b + 2 * (g // 4 + 1)) % bands * grids + g, b * grids + g))
    return pairs


def gather_block(slab):
    base = jnp.concatenate([slab, ring(slab, "grid", partner)], axis=1)
    up, down = [base], [base]
    for _ in range(3):
        up.append(ring(up[-1], "grid", above))
        down.append(ring(down[-1], "grid", below))
    far = jnp.concatenate([ring(up[3][:2], "grid", above), ring(down[3][2:], "grid", below)], axis=0)
    return jnp.concatenate(up + [far] + down[:0:-1], axis=1)


def scatter_block(total):
    part = [total[:, 6 * k:6 * k + 6] for k in range(8)]
    up = ring(part[4][:2], "grid", below)
    down = ring(part[4][2:], "grid", above)
    up = jnp.concatenate([part[3][:2] + up, part[3][2:]], axis=0)
    down = jnp.concatenate([part[5][:2], part[5][2:] + down], axis=0)
    for k in (2, 1):
        up = part[k] + ring(up, "grid", below)
        down = part[8 - k] + ring(down, "grid", above)
    both = part[0] + ring(up, "grid", below) + ring(down, "grid", above)
    return both[:, :3] + ring(both[:, 3:], "grid", partner)


def on_device(orbitals, occupation, cutoff):
    weights = occupation.astype(jnp.float32) * -0.5
    g = lax.axis_index("grid")
    gi, gj = g // 4, g % 4
    route = visit_route()
    axes = ("band", "grid")

    w_mine = lax.dynamic_slice(weights, (gj,), (1,))
    w_visit = lax.ppermute(w_mine, axes, route)
    w_oth = ring(w_mine, "band", twin)
    w_next = ring(w_visit, "band", twin)
    w_back = jnp.where(gi == 3, jnp.zeros_like(weights), weights)
    wts = jnp.concatenate([w_back, w_visit, w_next, w_mine, w_oth])

    own = gather_block(orbitals)
    lent = lax.dynamic_slice(own, (gj, 0, 0), (1, G, G * G))
    first = lax.ppermute(lent, axes, route)
    oth = ring(lent, "band", twin)
    vis = jnp.concatenate([first, ring(first, "band", twin)], axis=0)

    z, y = g % 8, g // 8
    r = jnp.arange(G, dtype=jnp.int32)
    place = 3 * (((y + r // 3 % 2) % 2) * 8 + (z + r // 6) % 8) + r % 3
    turned = basis(place)
    plain = basis(r)
    home, back = pair_solver(
        jnp.stack([gi, gj]), wts, own, vis, oth, kernel_table(cutoff),
        stacked(turned), stacked(turned.T), stacked(plain), stacked(plain.T),
    )
    mine = back[:1] + ring(back[1:], "band", twin)
    mine = lax.ppermute(mine, axes, [(d, s) for s, d in route])
    old = lax.dynamic_slice(home, (gj, 0, 0), (1, G, G * G))
    home = lax.dynamic_update_slice(home, old + mine, (gj, 0, 0))
    return scatter_block(home)


def solution(mesh):
    placed = (P("band", "grid", None), P("band"), P())
    return jax.shard_map(
        on_device, mesh=mesh, in_specs=placed, out_specs=P("band", "grid", None), check_vma=False
    )
```

```python
import numpy as np
import jax
import jax.numpy as jnp
from jax import lax
from jax.experimental import pallas as pl
from jax.experimental.pallas import tpu as pltpu
from jax.sharding import PartitionSpec as P


G = 48
ROW = G * G
HALF = ROW // 2
SLOTS = 9
WIDE = 512
YB = 8
LB = YB * G
VM = pl.BlockSpec(memory_space=pltpu.VMEM)
SM = pl.BlockSpec(memory_space=pltpu.SMEM)


def split2(x):
    hi = x.astype(jnp.bfloat16)
    lo = (x - hi.astype(jnp.float32)).astype(jnp.bfloat16)
    return jnp.concatenate([hi, lo], axis=0)


def apply(mat, x):
    both = jnp.dot(mat, split2(x), preferred_element_type=jnp.float32)
    return both[:G] + both[G:]


def f32(*shape):
    return jax.ShapeDtypeStruct(shape, jnp.float32)


def small_call(body, outs, *args, scalars=0):
    many = len(outs) > 1
    return pl.pallas_call(
        body,
        out_shape=outs if many else outs[0],
        in_specs=[SM] * scalars + [VM] * (len(args) - scalars),
        out_specs=[VM] * len(outs) if many else VM,
        cost_estimate=pl.CostEstimate(flops=10**6, bytes_accessed=10**6, transcendentals=0),
    )(*args)


def pack_body(y, slab, came, blk):
    flip = y[0] != 0
    for o in range(2):
        mine = slab[2 * y[0] + o]
        other = came[o]
        a = jnp.where(flip, other, mine)
        b = jnp.where(flip, mine, other)
        for h in range(2):
            r = o * 12 + h * 6
            blk[r:r + 3, :] = a[:, h * HALF:(h + 1) * HALF]
            blk[r + 3:r + 6, :] = b[:, h * HALF:(h + 1) * HALF]


def assemble_body(*refs):
    out = refs[-1]
    for k in range(8):
        for o in range(2):
            for h in range(2):
                r = o * 12 + h * 6
                out[o, 6 * k:6 * k + 6, h * HALF:(h + 1) * HALF] = refs[k][r:r + 6, :]


def disperse_body(a, b, c, *outs):
    for k in range(8):
        for o in range(2):
            for h in range(2):
                r = o * 12 + h * 6
                rows, lanes = slice(6 * k, 6 * k + 6), slice(h * HALF, (h + 1) * HALF)
                outs[k][r:r + 6, :] = a[o, rows, lanes] + b[o, rows, lanes] + c[o, rows, lanes]


def unpack_body(y, s, keep, give):
    flip = y[0] != 0
    for o in range(2):
        for h in range(2):
            r = o * 12 + h * 6
            a, b = s[r:r + 3, :], s[r + 3:r + 6, :]
            keep[o, :, h * HALF:(h + 1) * HALF] = jnp.where(flip, b, a)
            give[o, :, h * HALF:(h + 1) * HALF] = jnp.where(flip, a, b)


def finish_body(y, keep, came, out):
    for o in range(2):
        out[2 * y[0] + o] = keep[o]
        out[2 * (1 - y[0]) + o] = came[o]


def kernel(idx, w_own, w_twin, w_vis, own, twin, vis, ktab, fx, ix, fz, iz, home, away, back, spec, rows, cols, zed):
    gi, gj, once = idx[0], idx[1], idx[2]

    def pick(i, lanes):
        return jnp.where(i < 2, own[i & 1, :, lanes], twin[i & 1, :, lanes])

    def ours(i, lanes):
        return own[i, :, lanes] if i < 2 else twin[i - 2, :, lanes]

    def enter(yb, _):
        lanes = pl.ds(pl.multiple_of(yb * LB, LB), LB)
        for p in range(SLOTS):
            if p < 8:
                r = ours(p % 4, lanes) * vis[p // 4, :, lanes]
            else:
                r = pick(gi, lanes) * pick(gj, lanes)
            rows[p * G:(p + 1) * G, :] = apply(fx[...], r)
        for c in range(3):
            cols[c * 128:(c + 1) * 128, :] = rows[:, c * 128:(c + 1) * 128].T
        for y in range(YB):
            zed[y] = apply(fz[...], cols[y * G:(y + 1) * G, :])
        spec[:, pl.ds(pl.multiple_of(yb * YB, YB), YB), :] = jnp.swapaxes(zed[...], 0, 1)
        return 0

    lax.fori_loop(0, G // YB, enter, 0)

    def middle(k, _):
        for u in range(2):
            kz = k * 2 + u
            t = ktab[kz]
            t = jnp.concatenate([t, t[:, :WIDE - LB]], axis=1)
            s = apply(fz[...], spec[kz]) * t
            spec[kz] = apply(iz[...], s)
        return 0

    lax.fori_loop(0, G // 2, middle, 0)

    keep = jnp.where(once != 0, 0.0, 1.0)
    wo = [w_own[0] * keep, w_own[1] * keep, w_twin[0] * keep, w_twin[1] * keep]
    wj = jnp.where(gj < 2, w_own[gj & 1], w_twin[gj & 1])
    wg = jnp.where(gi < 2, wj, 0.0)
    wt = jnp.where(gi < 2, 0.0, wj)

    def leave(yb, _):
        lanes = pl.ds(pl.multiple_of(yb * LB, LB), LB)
        zed[...] = jnp.swapaxes(spec[:, pl.ds(pl.multiple_of(yb * YB, YB), YB), :], 0, 1)
        for y in range(YB):
            cols[y * G:(y + 1) * G, :] = apply(iz[...], zed[y])
        for c in range(3):
            rows[:, c * 128:(c + 1) * 128] = cols[c * 128:(c + 1) * 128, :].T
        b0 = None
        b1 = None
        v0 = vis[0, :, lanes] * w_vis[0]
        v1 = vis[1, :, lanes] * w_vis[1]
        for i in range(4):
            p0 = apply(ix[...], rows[i * G:(i + 1) * G, :])
            p1 = apply(ix[...], rows[(i + 4) * G:(i + 5) * G, :])
            (home if i < 2 else away)[i % 2, :, lanes] = v0 * p0 + v1 * p1
            o = ours(i, lanes) * wo[i]
            b0 = o * p0 if b0 is None else b0 + o * p0
            b1 = o * p1 if b1 is None else b1 + o * p1
        back[0, :, lanes] = b0
        back[1, :, lanes] = b1
        p8 = pick(gj, lanes) * apply(ix[...], rows[8 * G:9 * G, :])
        home[gi & 1, :, lanes] = home[gi & 1, :, lanes] + p8 * wg
        away[gi & 1, :, lanes] = away[gi & 1, :, lanes] + p8 * wt
        return 0

    lax.fori_loop(0, G // YB, leave, 0)


def pair_solver(*args):
    return pl.pallas_call(
        kernel,
        out_shape=[f32(2, G, ROW)] * 3,
        in_specs=[SM] * 4 + [VM] * 8,
        out_specs=[VM] * 3,
        scratch_shapes=[
            pltpu.VMEM((G, G, WIDE), jnp.float32),
            pltpu.VMEM((WIDE, LB), jnp.float32),
            pltpu.VMEM((LB, WIDE), jnp.float32),
            pltpu.VMEM((YB, G, WIDE), jnp.float32),
        ],
        compiler_params=pltpu.CompilerParams(vmem_limit_bytes=48 << 20),
        cost_estimate=pl.CostEstimate(flops=10**10, bytes_accessed=10**7, transcendentals=0),
    )(*args)


def stacked(m):
    top = lax.reduce_precision(m, 8, 7)
    hi = top.astype(jnp.bfloat16)
    lo = (m - top).astype(jnp.bfloat16)
    return jnp.concatenate([jnp.concatenate([hi, hi], 1), jnp.concatenate([lo, jnp.zeros_like(lo)], 1)], 0)


def plain_basis():
    k = np.arange(G)
    m = np.where(k <= G // 2, k, k - G // 2)
    ang = (2.0 * np.pi / G) * (m[:, None] * k[None, :] % G)
    return np.where((k <= G // 2)[:, None], np.cos(ang), np.sin(ang)).astype(np.float32)


def basis(place):
    k = jnp.arange(G, dtype=jnp.int32)
    m = jnp.where(k <= G // 2, k, k - G // 2)
    ang = (2.0 * np.pi / G) * ((m[:, None] * place[None, :]) % G).astype(jnp.float32)
    return jnp.where((k <= G // 2)[:, None], jnp.cos(ang), jnp.sin(ang))


def kernel_table(cutoff):
    def freq(shape, dim):
        k = lax.broadcasted_iota(jnp.int32, shape, dim) % G
        m = jnp.where(k <= G // 2, k, k - G // 2)
        return m * m, jnp.where((k == 0) | (k == G // 2), 1.0, 2.0)
    (a, wa), (b, wb), (c, wc) = freq((G, 1, 1), 0), freq((1, G, 1), 1), freq((1, 1, LB), 2)
    n = a + b + c
    ratios = n.astype(jnp.float32) * 0.5
    screen = jnp.where(n > 0, (1.0 - jnp.exp(-ratios)) / jnp.maximum(ratios, 0.5), 1.0)
    return jnp.where(n <= cutoff, 4.0 * screen * (wa * wb * wc / float(G**3)), 0.0)


def ring(block, axis, source):
    return lax.ppermute(block, axis, [(source(i), i) for i in range(lax.axis_size(axis))])


def partner(i):
    return (i + 8) % 16


def along(k):
    return lambda i: i // 8 * 8 + (i + k) % 8


def twin_of(i):
    return i ^ 1


OFFSETS = ((1, 0), (0, 1), (1, 1), (1, 3), (2, 3), (3, 2), None, (2, 2))
CLASSES = ((0, 5, 1, 4, 2, 3, 6, 7), (5, 0, 4, 1, 3, 2, 7, 6))


def source_chip(kind, x, y):
    if kind == 6:
        px, py = x // 2, y // 2
        px, py = {(0, 0): (1, 0), (1, 0): (1, 1), (1, 1): (0, 1), (0, 1): (0, 0)}[(px, py)]
        return px * 2 + x % 2, py * 2 + y % 2
    dx, dy = OFFSETS[kind]
    return (x + dx) % 4, (y + dy) % 4


def visit_route():
    pairs = []
    for b in range(16):
        for g in range(16):
            core, z = b % 2, g % 8
            x, y = source_chip(CLASSES[core][z], b // 2 % 4, g // 8 * 2 + b // 8)
            pairs.append(((((y % 2) * 4 + x) * 2 + core) * 16 + y // 2 * 8 + z, b * 16 + g))
    return pairs


def gather_blocks(b0):
    got = {0: b0}
    for k in (2, 6, 1, 7):
        got[k] = ring(b0, "grid", along(k))
    got[3] = ring(got[2], "grid", along(1))
    got[5] = ring(got[6], "grid", along(7))
    far = ring(got[2][:8], "grid", along(2))
    rest = ring(got[6][8:], "grid", along(6))
    got[4] = jnp.concatenate([far, rest], axis=0)
    return [got[k] for k in range(8)]


def scatter_blocks(part):
    total = part[0]
    came = [ring(part[k], "grid", along(-k)) for k in (4, 3, 5, 2, 6, 1, 7)]
    for c in came[::-1]:
        total = total + c
    return total


def on_device(orbitals, occupation, cutoff):
    axes = ("band", "grid")
    g = lax.axis_index("grid")
    core = lax.axis_index("band") % 2
    z, y = g % 8, g // 8
    y1 = y.reshape(1)
    route = visit_route()
    give = lax.dynamic_slice(orbitals, (2 * (1 - y), 0, 0), (2, 3, ROW))
    came = ring(give, "grid", partner)
    blk = small_call(pack_body, [f32(24, HALF)], y1, orbitals, came, scalars=1)
    got = gather_blocks(blk)
    own = small_call(assemble_body, [f32(2, G, ROW)], *got)
    vis = lax.ppermute(own, axes, route)
    twin = ring(own, "band", twin_of)

    late = lax.optimization_barrier((occupation, blk))[0]
    weights = late.astype(jnp.float32) * -0.5
    w_own = lax.dynamic_slice(weights, (2 * y,), (2,))
    w_twin = ring(w_own, "band", twin_of)
    w_vis = lax.ppermute(w_own, axes, route)

    e = z * 2 + core
    once = jnp.where(z == 7 - core, 1, 0)
    idx = jnp.stack([e // 4 ^ 2 * core, e % 4 ^ 2 * core, once])
    r = jnp.arange(G, dtype=jnp.int32)
    turned = basis(3 * (r // 3 % 2 * 8 + (z + r // 6) % 8) + r % 3)
    plain = jnp.asarray(plain_basis())
    home, away, back = pair_solver(
        idx, w_own, w_twin, w_vis, own, twin, vis, kernel_table(cutoff),
        stacked(turned), stacked(turned.T), stacked(plain), stacked(plain.T),
    )
    returned = lax.ppermute(back, axes, [(d, s) for s, d in route])
    swapped = ring(away, "band", twin_of)
    part = small_call(disperse_body, [f32(24, HALF)] * 8, home, swapped, returned)
    total = scatter_blocks(part)
    keep, give = small_call(unpack_body, [f32(2, 3, ROW)] * 2, y1, total, scalars=1)
    came = ring(give, "grid", partner)
    return small_call(finish_body, [f32(4, 3, ROW)], y1, keep, came, scalars=1)


def solution(mesh):
    placed = (P("band", "grid", None), P("band"), P())
    return jax.shard_map(
        on_device, mesh=mesh, in_specs=placed, out_specs=P("band", "grid", None), check_vma=False
    )
```

```python
import functools

import numpy as np
import jax
import jax.numpy as jnp
from jax import lax
from jax.experimental import pallas as pl
from jax.experimental.pallas import tpu as pltpu
from jax.sharding import PartitionSpec as P


G = 48
ROW = G * G
HALF = ROW // 2
WIDE = 256
YB = 8
LB = YB * G
VM = pl.BlockSpec(memory_space=pltpu.VMEM)
SM = pl.BlockSpec(memory_space=pltpu.SMEM)


def split2(x):
    hi = x.astype(jnp.bfloat16)
    lo = (x - hi.astype(jnp.float32)).astype(jnp.bfloat16)
    return jnp.concatenate([hi, lo], axis=0)


def apply(mat, x):
    both = jnp.dot(mat, split2(x), preferred_element_type=jnp.float32)
    return both[:G] + both[G:]


def f32(*shape):
    return jax.ShapeDtypeStruct(shape, jnp.float32)


def small_call(body, outs, *args, scalars=0):
    many = len(outs) > 1
    return pl.pallas_call(
        body,
        out_shape=outs if many else outs[0],
        in_specs=[SM] * scalars + [VM] * (len(args) - scalars),
        out_specs=[VM] * len(outs) if many else VM,
        cost_estimate=pl.CostEstimate(flops=10**6, bytes_accessed=10**6, transcendentals=0),
    )(*args)


def pack_body(y, slab, came, blk):
    flip = y[0] != 0
    for o in range(2):
        mine = slab[2 * y[0] + o]
        other = came[o]
        a = jnp.where(flip, other, mine)
        b = jnp.where(flip, mine, other)
        for h in range(2):
            r = o * 12 + h * 6
            blk[r:r + 3, :] = a[:, h * HALF:(h + 1) * HALF]
            blk[r + 3:r + 6, :] = b[:, h * HALF:(h + 1) * HALF]


def assemble_body(*refs):
    both, lone = refs[8], refs[9:]
    for k in range(8):
        for o in range(2):
            for h in range(2):
                r = o * 12 + h * 6
                rows, lanes = slice(6 * k, 6 * k + 6), slice(h * HALF, (h + 1) * HALF)
                piece = refs[k][r:r + 6, :]
                both[o, rows, lanes] = piece
                lone[o][rows, lanes] = piece


def disperse_body(a, b, c0, c1, *outs):
    back = (c0, c1)
    for k in range(8):
        for o in range(2):
            for h in range(2):
                r = o * 12 + h * 6
                rows, lanes = slice(6 * k, 6 * k + 6), slice(h * HALF, (h + 1) * HALF)
                outs[k][r:r + 6, :] = a[o, rows, lanes] + b[o, rows, lanes] + back[o][rows, lanes]


def unpack_body(y, *refs):
    keep, give = refs[8:]
    flip = y[0] != 0
    for o in range(2):
        for h in range(2):
            r = o * 12 + h * 6
            total = refs[0][r:r + 6, :]
            for k in range(1, 8):
                total = total + refs[k][r:r + 6, :]
            a, b = total[:3], total[3:]
            keep[o, :, h * HALF:(h + 1) * HALF] = jnp.where(flip, b, a)
            give[o, :, h * HALF:(h + 1) * HALF] = jnp.where(flip, a, b)


def kernel(first, idx, w_own, w_twin, w_vis, own, twin, vis, ktab, fx, ix, fz, iz, *refs):
    prior = () if first else refs[:2]
    home, away, back, spec, rows, cols, zed = refs[len(prior):]
    gi, gj = idx[0], idx[1]
    once = idx[2] if first else idx[3]
    slots = 5 if first else 4

    def pick(i, lanes):
        return jnp.where(i < 2, own[i & 1, :, lanes], twin[i & 1, :, lanes])

    def ours(i, lanes):
        return own[i, :, lanes] if i < 2 else twin[i - 2, :, lanes]

    def enter(yb, _):
        lanes = pl.ds(pl.multiple_of(yb * LB, LB), LB)
        for p in range(slots):
            r = ours(p, lanes) * vis[:, lanes] if p < 4 else pick(gi, lanes) * pick(gj, lanes)
            rows[p * G:(p + 1) * G, :] = apply(fx[...], r)
        for c in range(3):
            cols[c * 128:(c + 1) * 128, :] = rows[:, c * 128:(c + 1) * 128].T
        for y in range(YB):
            zed[y] = apply(fz[...], cols[y * G:(y + 1) * G, :])
        spec[:, pl.ds(pl.multiple_of(yb * YB, YB), YB), :] = jnp.swapaxes(zed[...], 0, 1)
        return 0

    lax.fori_loop(0, G // YB, enter, 0)

    def middle(k, _):
        for u in range(4):
            kz = k * 4 + u
            s = apply(fz[...], spec[kz]) * ktab[kz]
            spec[kz] = apply(iz[...], s)
        return 0

    lax.fori_loop(0, G // 4, middle, 0)

    keep = jnp.where(once != 0, 0.0, 1.0)
    wo = [w_own[0] * keep, w_own[1] * keep, w_twin[0] * keep, w_twin[1] * keep]
    wj = jnp.where(gj < 2, w_own[gj & 1], w_twin[gj & 1])
    wg = jnp.where(gi < 2, wj, 0.0)
    wt = jnp.where(gi < 2, 0.0, wj)

    def leave(yb, _):
        lanes = pl.ds(pl.multiple_of(yb * LB, LB), LB)
        zed[...] = jnp.swapaxes(spec[:, pl.ds(pl.multiple_of(yb * YB, YB), YB), :], 0, 1)
        for y in range(YB):
            cols[y * G:(y + 1) * G, :] = apply(iz[...], zed[y])
        for c in range(3):
            rows[:, c * 128:(c + 1) * 128] = cols[c * 128:(c + 1) * 128, :].T
        total = None
        v = vis[:, lanes] * w_vis[0]
        for i in range(4):
            p = apply(ix[...], rows[i * G:(i + 1) * G, :])
            side = i // 2
            term = v * p
            if not first:
                term = term + prior[side][i % 2, :, lanes]
            (home, away)[side][i % 2, :, lanes] = term
            o = ours(i, lanes) * wo[i] * p
            total = o if total is None else total + o
        back[:, lanes] = total
        if first:
            p = pick(gj, lanes) * apply(ix[...], rows[4 * G:5 * G, :])
            home[gi & 1, :, lanes] = home[gi & 1, :, lanes] + p * wg
            away[gi & 1, :, lanes] = away[gi & 1, :, lanes] + p * wt
        return 0

    lax.fori_loop(0, G // YB, leave, 0)


def pair_solver(first, *args):
    return pl.pallas_call(
        functools.partial(kernel, first),
        out_shape=[f32(2, G, ROW), f32(2, G, ROW), f32(G, ROW)],
        in_specs=[SM] * 4 + [VM] * (len(args) - 4),
        out_specs=[VM] * 3,
        scratch_shapes=[
            pltpu.VMEM((G, G, WIDE), jnp.float32),
            pltpu.VMEM((WIDE, LB), jnp.float32),
            pltpu.VMEM((LB, WIDE), jnp.float32),
            pltpu.VMEM((YB, G, WIDE), jnp.float32),
        ],
        compiler_params=pltpu.CompilerParams(vmem_limit_bytes=40 << 20),
        cost_estimate=pl.CostEstimate(flops=5 * 10**9, bytes_accessed=10**7, transcendentals=0),
    )(*args)


def stacked(m):
    top = lax.reduce_precision(m, 8, 7)
    hi = top.astype(jnp.bfloat16)
    lo = (m - top).astype(jnp.bfloat16)
    return jnp.concatenate([jnp.concatenate([hi, hi], 1), jnp.concatenate([lo, jnp.zeros_like(lo)], 1)], 0)


def plain_basis():
    k = np.arange(G)
    m = np.where(k <= G // 2, k, k - G // 2)
    ang = (2.0 * np.pi / G) * (m[:, None] * k[None, :] % G)
    return np.where((k <= G // 2)[:, None], np.cos(ang), np.sin(ang)).astype(np.float32)


def basis(place):
    k = jnp.arange(G, dtype=jnp.int32)
    m = jnp.where(k <= G // 2, k, k - G // 2)
    ang = (2.0 * np.pi / G) * ((m[:, None] * place[None, :]) % G).astype(jnp.float32)
    return jnp.where((k <= G // 2)[:, None], jnp.cos(ang), jnp.sin(ang))


def kernel_table(cutoff):
    def freq(shape, dim):
        k = lax.broadcasted_iota(jnp.int32, shape, dim) % G
        m = jnp.where(k <= G // 2, k, k - G // 2)
        return m * m, jnp.where((k == 0) | (k == G // 2), 1.0, 2.0)
    (a, wa), (b, wb), (c, wc) = freq((G, 1, 1), 0), freq((1, G, 1), 1), freq((1, 1, WIDE), 2)
    n = a + b + c
    ratios = n.astype(jnp.float32) * 0.5
    screen = jnp.where(n > 0, (1.0 - jnp.exp(-ratios)) / jnp.maximum(ratios, 0.5), 1.0)
    return jnp.where(n <= cutoff, 4.0 * screen * (wa * wb * wc / float(G**3)), 0.0)


def ring(block, axis, source):
    return lax.ppermute(block, axis, [(source(i), i) for i in range(lax.axis_size(axis))])


def partner(i):
    return (i + 8) % 16


def along(k):
    return lambda i: i // 8 * 8 + (i + k) % 8


def twin_of(i):
    return i ^ 1


OFFSETS = ((1, 0), (0, 1), (1, 1), (1, 3), (2, 1), (3, 2), None, (2, 0))
ORDER = ((2, 4, 6, 7, 0, 1, 3, 5), (0, 1, 3, 5, 2, 4, 6, 7))
MATCH = (5, 3, 2, 1, 4, 0, 6, 7)


def class_of(core, z, v):
    kind = ORDER[v][z]
    return MATCH[kind] if core else kind


def source_chip(kind, x, y):
    if kind == 6:
        px, py = x // 2, y // 2
        px, py = {(0, 0): (0, 1), (0, 1): (1, 0), (1, 0): (1, 1), (1, 1): (0, 0)}[(px, py)]
        return px * 2 + x % 2, py * 2 + y % 2
    dx, dy = OFFSETS[kind]
    return (x + dx) % 4, (y + dy) % 4


def visit_route(v, both_ways=True):
    pairs = []
    for b in range(16):
        for g in range(16):
            core, z = b % 2, g % 8
            kind = class_of(core, z, v)
            x, y = source_chip(kind, b // 2 % 4, g // 8 * 2 + b // 8)
            if both_ways or kind != 7:
                pairs.append(((((y % 2) * 4 + x) * 2 + core) * 16 + y // 2 * 8 + z, b * 16 + g))
    return pairs


def returned(back, v):
    return lax.ppermute(back, ("band", "grid"), [(d, s) for s, d in visit_route(v, False)])


def gather_blocks(b0):
    got = {0: b0}
    for k in (2, 6, 1, 7):
        got[k] = ring(b0, "grid", along(k))
    got[3] = ring(got[2], "grid", along(1))
    got[5] = ring(got[6], "grid", along(7))
    far = ring(got[2][:8], "grid", along(2))
    rest = ring(got[6][8:], "grid", along(6))
    got[4] = jnp.concatenate([far, rest], axis=0)
    return [got[k] for k in range(8)]


def scatter_blocks(part):
    return [part[0]] + [ring(part[k], "grid", along(-k)) for k in (4, 3, 5, 2, 6, 1, 7)]


def on_device(orbitals, occupation, cutoff):
    axes = ("band", "grid")
    g = lax.axis_index("grid")
    core = lax.axis_index("band") % 2
    z, y = g % 8, g // 8
    y1 = y.reshape(1)
    give = lax.dynamic_slice(orbitals, (2 * (1 - y), 0, 0), (2, 3, ROW))
    came = ring(give, "grid", partner)
    blk = small_call(pack_body, [f32(24, HALF)], y1, orbitals, came, scalars=1)

    late = lax.optimization_barrier((occupation, blk))[0]
    weights = late.astype(jnp.float32) * -0.5
    w_own = lax.dynamic_slice(weights, (2 * y,), (2,))
    w_twin = ring(w_own, "band", twin_of)
    w_vis = [lax.ppermute(w_own[v:v + 1], axes, visit_route(v)) for v in range(2)]

    got = gather_blocks(blk)
    got, w_twin, w_vis = lax.optimization_barrier((got, w_twin, w_vis))
    own, *lone = small_call(assemble_body, [f32(2, G, ROW), f32(G, ROW), f32(G, ROW)], *got)
    twin = ring(own, "band", twin_of)
    vis = [lax.ppermute(lone[v], axes, visit_route(v)) for v in range(2)]

    e = z * 2 + core
    once = [z == ORDER[v].index(7) for v in range(2)]
    idx = jnp.stack([e // 4 ^ 2 * core, e % 4 ^ 2 * core] + [o.astype(jnp.int32) for o in once])
    r = jnp.arange(G, dtype=jnp.int32)
    turned = basis(3 * (r // 3 % 2 * 8 + (z + r // 6) % 8) + r % 3)
    plain = jnp.asarray(plain_basis())
    tables = (kernel_table(cutoff), stacked(turned), stacked(turned.T), stacked(plain), stacked(plain.T))
    home, away, back = pair_solver(True, idx, w_own, w_twin, w_vis[0], own, twin, vis[0], *tables)
    ret0 = returned(back, 0)
    home, away, back = pair_solver(False, idx, w_own, w_twin, w_vis[1], own, twin, vis[1], *tables, home, away)
    ret1 = returned(back, 1)
    swapped = ring(away, "band", twin_of)
    part = small_call(disperse_body, [f32(24, HALF)] * 8, home, swapped, ret0, ret1)
    keep, give = small_call(unpack_body, [f32(2, 3, ROW)] * 2, y1, *scatter_blocks(part), scalars=1)
    came = ring(give, "grid", partner)
    return jnp.concatenate([jnp.where(y == 0, keep, came), jnp.where(y == 0, came, keep)], axis=0)


def solution(mesh):
    placed = (P("band", "grid", None), P("band"), P())
    return jax.shard_map(
        on_device, mesh=mesh, in_specs=placed, out_specs=P("band", "grid", None), check_vma=False
    )
```

```python
import functools

import numpy as np
import jax
import jax.numpy as jnp
from jax import lax
from jax.experimental import pallas as pl
from jax.experimental.pallas import tpu as pltpu
from jax.sharding import PartitionSpec as P


G = 48
ROW = G * G
HALF = ROW // 2
WIDE = 256
YB = 8
LB = YB * G
VM = pl.BlockSpec(memory_space=pltpu.VMEM)
SM = pl.BlockSpec(memory_space=pltpu.SMEM)


def split2(x):
    hi = x.astype(jnp.bfloat16)
    lo = (x - hi.astype(jnp.float32)).astype(jnp.bfloat16)
    return jnp.concatenate([hi, lo], axis=0)


def apply(mat, x):
    both = jnp.dot(mat, split2(x), preferred_element_type=jnp.float32)
    return both[:G] + both[G:]


def f32(*shape):
    return jax.ShapeDtypeStruct(shape, jnp.float32)


def small_call(body, outs, *args, scalars=0):
    many = len(outs) > 1
    return pl.pallas_call(
        body,
        out_shape=outs if many else outs[0],
        in_specs=[SM] * scalars + [VM] * (len(args) - scalars),
        out_specs=[VM] * len(outs) if many else VM,
        cost_estimate=pl.CostEstimate(flops=10**6, bytes_accessed=10**6, transcendentals=0),
    )(*args)


def pack_body(y, slab, came, blk):
    flip = y[0] != 0
    for o in range(2):
        mine = slab[2 * y[0] + o]
        other = came[o]
        a = jnp.where(flip, other, mine)
        b = jnp.where(flip, mine, other)
        for h in range(2):
            r = o * 12 + h * 6
            blk[r:r + 3, :] = a[:, h * HALF:(h + 1) * HALF]
            blk[r + 3:r + 6, :] = b[:, h * HALF:(h + 1) * HALF]


def assemble_body(*refs):
    both, lone = refs[8], refs[9:]
    for k in range(8):
        for o in range(2):
            for h in range(2):
                r = o * 12 + h * 6
                rows, lanes = slice(6 * k, 6 * k + 6), slice(h * HALF, (h + 1) * HALF)
                piece = refs[k][r:r + 6, :]
                both[o, rows, lanes] = piece
                lone[o][rows, lanes] = piece


def disperse_body(a, b, c0, c1, *outs):
    back = (c0, c1)
    for k in range(8):
        for o in range(2):
            for h in range(2):
                r = o * 12 + h * 6
                rows, lanes = slice(6 * k, 6 * k + 6), slice(h * HALF, (h + 1) * HALF)
                outs[k][r:r + 6, :] = a[o, rows, lanes] + b[o, rows, lanes] + back[o][rows, lanes]


def unpack_body(y, *refs):
    keep, give = refs[8:]
    flip = y[0] != 0
    for o in range(2):
        for h in range(2):
            r = o * 12 + h * 6
            total = refs[0][r:r + 6, :]
            for k in range(1, 8):
                total = total + refs[k][r:r + 6, :]
            a, b = total[:3], total[3:]
            keep[o, :, h * HALF:(h + 1) * HALF] = jnp.where(flip, b, a)
            give[o, :, h * HALF:(h + 1) * HALF] = jnp.where(flip, a, b)


def kernel(first, idx, w_own, w_twin, w_vis, own, twin, vis, ktab, fx, ix, fz, iz, *refs):
    prior = () if first else refs[:2]
    home, away, back, spec, rows, cols, zed = refs[len(prior):]
    gi, gj = idx[0], idx[1]
    once = idx[2] if first else idx[3]
    slots = 5 if first else 4

    def pick(i, lanes):
        return jnp.where(i < 2, own[i & 1, :, lanes], twin[i & 1, :, lanes])

    def ours(i, lanes):
        return own[i, :, lanes] if i < 2 else twin[i - 2, :, lanes]

    def enter(yb, _):
        lanes = pl.ds(pl.multiple_of(yb * LB, LB), LB)
        for p in range(slots):
            r = ours(p, lanes) * vis[:, lanes] if p < 4 else pick(gi, lanes) * pick(gj, lanes)
            rows[p * G:(p + 1) * G, :] = apply(fx[...], r)
        for c in range(3):
            cols[c * 128:(c + 1) * 128, :] = rows[:, c * 128:(c + 1) * 128].T
        for y in range(YB):
            zed[y] = apply(fz[...], cols[y * G:(y + 1) * G, :])
        spec[:, pl.ds(pl.multiple_of(yb * YB, YB), YB), :] = jnp.swapaxes(zed[...], 0, 1)
        return 0

    lax.fori_loop(0, G // YB, enter, 0)

    def middle(k, _):
        for u in range(4):
            kz = k * 4 + u
            s = apply(fz[...], spec[kz]) * ktab[kz]
            spec[kz] = apply(iz[...], s)
        return 0

    lax.fori_loop(0, G // 4, middle, 0)

    keep = jnp.where(once != 0, 0.0, 1.0)
    wo = [w_own[0] * keep, w_own[1] * keep, w_twin[0] * keep, w_twin[1] * keep]
    wj = jnp.where(gj < 2, w_own[gj & 1], w_twin[gj & 1])
    wg = jnp.where(gi < 2, wj, 0.0)
    wt = jnp.where(gi < 2, 0.0, wj)

    def leave(yb, _):
        lanes = pl.ds(pl.multiple_of(yb * LB, LB), LB)
        zed[...] = jnp.swapaxes(spec[:, pl.ds(pl.multiple_of(yb * YB, YB), YB), :], 0, 1)
        for y in range(YB):
            cols[y * G:(y + 1) * G, :] = apply(iz[...], zed[y])
        for c in range(3):
            rows[:, c * 128:(c + 1) * 128] = cols[c * 128:(c + 1) * 128, :].T
        total = None
        v = vis[:, lanes] * w_vis[0]
        for i in range(4):
            p = apply(ix[...], rows[i * G:(i + 1) * G, :])
            side = i // 2
            term = v * p
            if not first:
                term = term + prior[side][i % 2, :, lanes]
            (home, away)[side][i % 2, :, lanes] = term
            o = ours(i, lanes) * wo[i] * p
            total = o if total is None else total + o
        back[:, lanes] = total
        if first:
            p = pick(gj, lanes) * apply(ix[...], rows[4 * G:5 * G, :])
            home[gi & 1, :, lanes] = home[gi & 1, :, lanes] + p * wg
            away[gi & 1, :, lanes] = away[gi & 1, :, lanes] + p * wt
        return 0

    lax.fori_loop(0, G // YB, leave, 0)


def pair_solver(first, *args):
    return pl.pallas_call(
        functools.partial(kernel, first),
        out_shape=[f32(2, G, ROW), f32(2, G, ROW), f32(G, ROW)],
        in_specs=[SM] * 4 + [VM] * (len(args) - 4),
        out_specs=[VM] * 3,
        scratch_shapes=[
            pltpu.VMEM((G, G, WIDE), jnp.float32),
            pltpu.VMEM((WIDE, LB), jnp.float32),
            pltpu.VMEM((LB, WIDE), jnp.float32),
            pltpu.VMEM((YB, G, WIDE), jnp.float32),
        ],
        compiler_params=pltpu.CompilerParams(vmem_limit_bytes=40 << 20),
        cost_estimate=pl.CostEstimate(flops=5 * 10**9, bytes_accessed=10**7, transcendentals=0),
    )(*args)


def stacked(m):
    top = lax.reduce_precision(m, 8, 7)
    hi = top.astype(jnp.bfloat16)
    lo = (m - top).astype(jnp.bfloat16)
    return jnp.concatenate([jnp.concatenate([hi, hi], 1), jnp.concatenate([lo, jnp.zeros_like(lo)], 1)], 0)


def plain_basis():
    k = np.arange(G)
    m = np.where(k <= G // 2, k, k - G // 2)
    ang = (2.0 * np.pi / G) * (m[:, None] * k[None, :] % G)
    return np.where((k <= G // 2)[:, None], np.cos(ang), np.sin(ang)).astype(np.float32)


def basis(place):
    k = jnp.arange(G, dtype=jnp.int32)
    m = jnp.where(k <= G // 2, k, k - G // 2)
    ang = (2.0 * np.pi / G) * ((m[:, None] * place[None, :]) % G).astype(jnp.float32)
    return jnp.where((k <= G // 2)[:, None], jnp.cos(ang), jnp.sin(ang))


def kernel_table(cutoff):
    def freq(shape, dim):
        k = lax.broadcasted_iota(jnp.int32, shape, dim) % G
        m = jnp.where(k <= G // 2, k, k - G // 2)
        return m * m, jnp.where((k == 0) | (k == G // 2), 1.0, 2.0)

    (a, wa), (b, wb), (c, wc) = freq((G, 1, 1), 0), freq((1, G, 1), 1), freq((1, 1, WIDE), 2)
    n = a + b + c
    ratios = n.astype(jnp.float32) * 0.5
    screen = jnp.where(n > 0, (1.0 - jnp.exp(-ratios)) / jnp.maximum(ratios, 0.5), 1.0)
    return jnp.where(n <= cutoff, 4.0 * screen * (wa * wb * wc / float(G**3)), 0.0)


def ring(block, axis, source):
    return lax.ppermute(block, axis, [(source(i), i) for i in range(lax.axis_size(axis))])


def partner(i):
    return (i + 8) % 16


def along(k):
    return lambda i: i // 8 * 8 + (i + k) % 8


def twin_of(i):
    return i ^ 1


OFFSETS = ((1, 0), (0, 1), (1, 1), (1, 3), (2, 1), (3, 2), None, (2, 0))
ORDER = ((2, 4, 6, 7, 0, 1, 3, 5), (0, 1, 3, 5, 2, 4, 6, 7))
MATCH = (5, 3, 2, 1, 4, 0, 6, 7)


def class_of(core, z, v):
    kind = ORDER[v][z]
    return MATCH[kind] if core else kind


def source_chip(kind, x, y):
    if kind == 6:
        px, py = x // 2, y // 2
        px, py = {(0, 0): (0, 1), (0, 1): (1, 0), (1, 0): (1, 1), (1, 1): (0, 0)}[(px, py)]
        return px * 2 + x % 2, py * 2 + y % 2
    dx, dy = OFFSETS[kind]
    return (x + dx) % 4, (y + dy) % 4


def visit_route(v, both_ways=True):
    pairs = []
    for b in range(16):
        for g in range(16):
            core, z = b % 2, g % 8
            kind = class_of(core, z, v)
            x, y = source_chip(kind, b // 2 % 4, g // 8 * 2 + b // 8)
            if both_ways or kind != 7:
                pairs.append(((((y % 2) * 4 + x) * 2 + core) * 16 + y // 2 * 8 + z, b * 16 + g))
    return pairs


def returned(back, v):
    return lax.ppermute(back, ("band", "grid"), [(d, s) for s, d in visit_route(v, False)])


def gather_blocks(b0):
    got = {0: b0}
    for k in (2, 6, 1, 7):
        got[k] = ring(b0, "grid", along(k))
    got[3] = ring(got[2], "grid", along(1))
    got[5] = ring(got[6], "grid", along(7))
    far = ring(got[2][:8], "grid", along(2))
    rest = ring(got[6][8:], "grid", along(6))
    got[4] = jnp.concatenate([far, rest], axis=0)
    return [got[k] for k in range(8)]


def scatter_blocks(part):
    return [part[0]] + [ring(part[k], "grid", along(-k)) for k in (4, 3, 5, 2, 6, 1, 7)]


def on_device(orbitals, occupation, cutoff):
    axes = ("band", "grid")
    g = lax.axis_index("grid")
    core = lax.axis_index("band") % 2
    z, y = g % 8, g // 8
    y1 = y.reshape(1)
    give = lax.dynamic_slice(orbitals, (2 * (1 - y), 0, 0), (2, 3, ROW))
    came = ring(give, "grid", partner)
    blk = small_call(pack_body, [f32(24, HALF)], y1, orbitals, came, scalars=1)

    got = gather_blocks(blk)
    own, *lone = small_call(assemble_body, [f32(2, G, ROW), f32(G, ROW), f32(G, ROW)], *got)
    first = lax.ppermute(lone[0], axes, visit_route(0))
    twin = ring(own, "band", twin_of)

    late = lax.optimization_barrier((occupation, own))[0]
    weights = late.astype(jnp.float32) * -0.5
    w_own = lax.dynamic_slice(weights, (2 * y,), (2,))
    w_twin = ring(w_own, "band", twin_of)
    w_first = lax.ppermute(w_own[:1], axes, visit_route(0))
    held, w_held, first = lax.optimization_barrier((lone[1], w_own[1:], first))
    second = lax.ppermute(held, axes, visit_route(1))
    w_second = lax.ppermute(w_held, axes, visit_route(1))

    e = z * 2 + core
    once = [z == ORDER[v].index(7) for v in range(2)]
    idx = jnp.stack([e // 4 ^ 2 * core, e % 4 ^ 2 * core] + [o.astype(jnp.int32) for o in once])
    r = jnp.arange(G, dtype=jnp.int32)
    turned = basis(3 * (r // 3 % 2 * 8 + (z + r // 6) % 8) + r % 3)
    plain = jnp.asarray(plain_basis())
    tables = (kernel_table(cutoff), stacked(turned), stacked(turned.T), stacked(plain), stacked(plain.T))
    home, away, back = pair_solver(True, idx, w_own, w_twin, w_first, own, twin, first, *tables)
    ret0 = returned(back, 0)
    home, away, back = pair_solver(False, idx, w_own, w_twin, w_second, own, twin, second, *tables, home, away)
    ret1 = returned(back, 1)
    swapped = ring(away, "band", twin_of)
    part = small_call(disperse_body, [f32(24, HALF)] * 8, home, swapped, ret0, ret1)
    keep, give = small_call(unpack_body, [f32(2, 3, ROW)] * 2, y1, *scatter_blocks(part), scalars=1)
    came = ring(give, "grid", partner)
    return jnp.concatenate([jnp.where(y == 0, keep, came), jnp.where(y == 0, came, keep)], axis=0)


def solution(mesh):
    placed = (P("band", "grid", None), P("band"), P())
    return jax.shard_map(
        on_device, mesh=mesh, in_specs=placed, out_specs=P("band", "grid", None), check_vma=False
    )
```

```python
import functools

import numpy as np
import jax
import jax.numpy as jnp
from jax import lax
from jax.experimental import pallas as pl
from jax.experimental.pallas import tpu as pltpu
from jax.sharding import PartitionSpec as P


G = 48
ROW = G * G
HALF = ROW // 2
WIDE = 256
YB = 8
LB = YB * G
VM = pl.BlockSpec(memory_space=pltpu.VMEM)
SM = pl.BlockSpec(memory_space=pltpu.SMEM)


def split2(x):
    hi = x.astype(jnp.bfloat16)
    lo = (x - hi.astype(jnp.float32)).astype(jnp.bfloat16)
    return jnp.concatenate([hi, lo], axis=0)


def apply(mat, x):
    both = jnp.dot(mat, split2(x), preferred_element_type=jnp.float32)
    return both[:G] + both[G:]


def f32(*shape):
    return jax.ShapeDtypeStruct(shape, jnp.float32)


def small_call(body, outs, *args, scalars=0):
    many = len(outs) > 1
    return pl.pallas_call(
        body,
        out_shape=outs if many else outs[0],
        in_specs=[SM] * scalars + [VM] * (len(args) - scalars),
        out_specs=[VM] * len(outs) if many else VM,
        compiler_params=pltpu.CompilerParams(vmem_limit_bytes=8 << 20),
        cost_estimate=pl.CostEstimate(flops=10**6, bytes_accessed=10**6, transcendentals=0),
    )(*args)


def pack_body(y, slab, came, blk):
    flip = y[0] != 0
    for o in range(2):
        mine = slab[2 * y[0] + o]
        other = came[o]
        a = jnp.where(flip, other, mine)
        b = jnp.where(flip, mine, other)
        for h in range(2):
            r = o * 12 + h * 6
            blk[r:r + 3, :] = a[:, h * HALF:(h + 1) * HALF]
            blk[r + 3:r + 6, :] = b[:, h * HALF:(h + 1) * HALF]


def assemble_body(*refs):
    both, lone = refs[8], refs[9:]
    for k in range(8):
        for o in range(2):
            for h in range(2):
                r = o * 12 + h * 6
                rows, lanes = slice(6 * k, 6 * k + 6), slice(h * HALF, (h + 1) * HALF)
                piece = refs[k][r:r + 6, :]
                both[o, rows, lanes] = piece
                lone[o][rows, lanes] = piece


def disperse_body(a, b, c0, c1, *outs):
    back = (c0, c1)
    for k in range(8):
        for o in range(2):
            for h in range(2):
                r = o * 12 + h * 6
                rows, lanes = slice(6 * k, 6 * k + 6), slice(h * HALF, (h + 1) * HALF)
                outs[k][r:r + 6, :] = a[o, rows, lanes] + b[o, rows, lanes] + back[o][rows, lanes]


def unpack_body(y, *refs):
    keep, give = refs[8:]
    flip = y[0] != 0
    for o in range(2):
        for h in range(2):
            r = o * 12 + h * 6
            total = refs[0][r:r + 6, :]
            for k in range(1, 8):
                total = total + refs[k][r:r + 6, :]
            a, b = total[:3], total[3:]
            keep[o, :, h * HALF:(h + 1) * HALF] = jnp.where(flip, b, a)
            give[o, :, h * HALF:(h + 1) * HALF] = jnp.where(flip, a, b)


def kernel(first, idx, w_own, w_twin, w_vis, own, twin, vis, ktab, fx, ix, fz, iz, *refs):
    prior = () if first else refs[:2]
    home, away, back, spec, *bufs = refs[len(prior):]
    gi, gj = idx[0], idx[1]
    once = idx[2] if first else idx[3]
    slots = 5 if first else 4

    def pick(i, lanes):
        return jnp.where(i < 2, own[i & 1, :, lanes], twin[i & 1, :, lanes])

    def ours(i, lanes):
        return own[i, :, lanes] if i < 2 else twin[i - 2, :, lanes]

    def enter_one(yb, rows, cols, zed):
        lanes = pl.ds(pl.multiple_of(yb * LB, LB), LB)
        for p in range(slots):
            r = ours(p, lanes) * vis[:, lanes] if p < 4 else pick(gi, lanes) * pick(gj, lanes)
            rows[p * G:(p + 1) * G, :] = apply(fx[...], r)
        for c in range(3):
            cols[c * 128:(c + 1) * 128, :] = rows[:, c * 128:(c + 1) * 128].T
        for y in range(YB):
            zed[y] = apply(fz[...], cols[y * G:(y + 1) * G, :])
        spec[:, pl.ds(pl.multiple_of(yb * YB, YB), YB), :] = jnp.swapaxes(zed[...], 0, 1)

    def enter(k, _):
        for u in range(3):
            enter_one(k * 3 + u, *bufs[u % 2 * 3:u % 2 * 3 + 3])
        return 0

    lax.fori_loop(0, G // YB // 3, enter, 0)

    def half_in(kz):
        return apply(fz[...], spec[kz]) * ktab[kz]

    for u in range(12):
        bufs[-1][u] = half_in(u)

    def middle(k, _):
        done = [apply(iz[...], bufs[-1][u]) for u in range(12)]
        for u in range(12):
            bufs[-1][u] = half_in((k + 1) * 12 + u)
        for u in range(12):
            spec[k * 12 + u] = done[u]
        return 0

    lax.fori_loop(0, G // 12 - 1, middle, 0)
    for u in range(12):
        spec[G - 12 + u] = apply(iz[...], bufs[-1][u])

    keep = jnp.where(once != 0, 0.0, 1.0)
    wo = [w_own[0] * keep, w_own[1] * keep, w_twin[0] * keep, w_twin[1] * keep]
    wj = jnp.where(gj < 2, w_own[gj & 1], w_twin[gj & 1])
    wg = jnp.where(gi < 2, wj, 0.0)
    wt = jnp.where(gi < 2, 0.0, wj)

    def leave_one(yb, rows, cols, zed):
        lanes = pl.ds(pl.multiple_of(yb * LB, LB), LB)
        zed[...] = jnp.swapaxes(spec[:, pl.ds(pl.multiple_of(yb * YB, YB), YB), :], 0, 1)
        for y in range(YB):
            cols[y * G:(y + 1) * G, :] = apply(iz[...], zed[y])
        for c in range(3):
            rows[:, c * 128:(c + 1) * 128] = cols[c * 128:(c + 1) * 128, :].T
        total = None
        v = vis[:, lanes] * w_vis[0]
        for i in range(4):
            p = apply(ix[...], rows[i * G:(i + 1) * G, :])
            side = i // 2
            term = v * p
            if not first:
                term = term + prior[side][i % 2, :, lanes]
            (home, away)[side][i % 2, :, lanes] = term
            o = ours(i, lanes) * wo[i] * p
            total = o if total is None else total + o
        back[:, lanes] = total
        if first:
            p = pick(gj, lanes) * apply(ix[...], rows[4 * G:5 * G, :])
            home[gi & 1, :, lanes] = home[gi & 1, :, lanes] + p * wg
            away[gi & 1, :, lanes] = away[gi & 1, :, lanes] + p * wt

    def leave(k, _):
        for u in range(3):
            leave_one(k * 3 + u, *bufs[u % 2 * 3:u % 2 * 3 + 3])
        return 0

    lax.fori_loop(0, G // YB // 3, leave, 0)


def pair_solver(first, *args):
    return pl.pallas_call(
        functools.partial(kernel, first),
        out_shape=[f32(2, G, ROW), f32(2, G, ROW), f32(G, ROW)],
        in_specs=[SM] * 4 + [VM] * (len(args) - 4),
        out_specs=[VM] * 3,
        scratch_shapes=[
            pltpu.VMEM((G, G, WIDE), jnp.float32),
        ] + [
            pltpu.VMEM((WIDE, LB), jnp.float32),
            pltpu.VMEM((LB, WIDE), jnp.float32),
            pltpu.VMEM((YB, G, WIDE), jnp.float32),
        ] * 2 + [pltpu.VMEM((12, G, WIDE), jnp.float32)],
        compiler_params=pltpu.CompilerParams(vmem_limit_bytes=24 << 20),
        cost_estimate=pl.CostEstimate(flops=5 * 10**9, bytes_accessed=10**7, transcendentals=0),
    )(*args)


def stacked(m):
    top = lax.reduce_precision(m, 8, 7)
    hi = top.astype(jnp.bfloat16)
    lo = (m - top).astype(jnp.bfloat16)
    return jnp.concatenate([jnp.concatenate([hi, hi], 1), jnp.concatenate([lo, jnp.zeros_like(lo)], 1)], 0)


def plain_basis():
    k = np.arange(G)
    m = np.where(k <= G // 2, k, k - G // 2)
    ang = (2.0 * np.pi / G) * (m[:, None] * k[None, :] % G)
    return np.where((k <= G // 2)[:, None], np.cos(ang), np.sin(ang)).astype(np.float32)


def basis(place):
    k = jnp.arange(G, dtype=jnp.int32)
    m = jnp.where(k <= G // 2, k, k - G // 2)
    ang = (2.0 * np.pi / G) * ((m[:, None] * place[None, :]) % G).astype(jnp.float32)
    return jnp.where((k <= G // 2)[:, None], jnp.cos(ang), jnp.sin(ang))


def kernel_table(cutoff):
    def freq(shape, dim):
        k = lax.broadcasted_iota(jnp.int32, shape, dim) % G
        m = jnp.where(k <= G // 2, k, k - G // 2)
        return m * m, jnp.where((k == 0) | (k == G // 2), 1.0, 2.0)

    (a, wa), (b, wb), (c, wc) = freq((G, 1, 1), 0), freq((1, G, 1), 1), freq((1, 1, WIDE), 2)
    n = a + b + c
    ratios = n.astype(jnp.float32) * 0.5
    screen = jnp.where(n > 0, (1.0 - jnp.exp(-ratios)) / jnp.maximum(ratios, 0.5), 1.0)
    return jnp.where(n <= cutoff, 4.0 * screen * (wa * wb * wc / float(G**3)), 0.0)


def ring(block, axis, source):
    return lax.ppermute(block, axis, [(source(i), i) for i in range(lax.axis_size(axis))])


def partner(i):
    return (i + 8) % 16


def along(k):
    return lambda i: i // 8 * 8 + (i + k) % 8


def twin_of(i):
    return i ^ 1


OFFSETS = ((1, 0), (0, 1), (1, 1), (1, 3), (2, 1), (3, 2), None, (2, 0))
ORDER = ((2, 4, 6, 7, 0, 1, 3, 5), (0, 1, 3, 5, 2, 4, 6, 7))
MATCH = (5, 3, 2, 1, 4, 0, 6, 7)


def class_of(core, z, v):
    kind = ORDER[v][z]
    return MATCH[kind] if core else kind


def source_chip(kind, x, y):
    if kind == 6:
        px, py = x // 2, y // 2
        px, py = {(0, 0): (0, 1), (0, 1): (1, 0), (1, 0): (1, 1), (1, 1): (0, 0)}[(px, py)]
        return px * 2 + x % 2, py * 2 + y % 2
    dx, dy = OFFSETS[kind]
    return (x + dx) % 4, (y + dy) % 4


def visit_route(v, both_ways=True):
    pairs = []
    for b in range(16):
        for g in range(16):
            core, z = b % 2, g % 8
            kind = class_of(core, z, v)
            x, y = source_chip(kind, b // 2 % 4, g // 8 * 2 + b // 8)
            if both_ways or kind != 7:
                pairs.append(((((y % 2) * 4 + x) * 2 + core) * 16 + y // 2 * 8 + z, b * 16 + g))
    return pairs


def returned(back, v):
    return lax.ppermute(back, ("band", "grid"), [(d, s) for s, d in visit_route(v, False)])


def gather_blocks(b0):
    got = {0: b0}
    for k in (2, 6, 1, 7):
        got[k] = ring(b0, "grid", along(k))
    got[3] = ring(got[2], "grid", along(1))
    got[5] = ring(got[6], "grid", along(7))
    far = ring(got[2][:8], "grid", along(2))
    rest = ring(got[6][8:], "grid", along(6))
    got[4] = jnp.concatenate([far, rest], axis=0)
    return [got[k] for k in range(8)]


def scatter_blocks(part):
    return [part[0]] + [ring(part[k], "grid", along(-k)) for k in (4, 3, 5, 2, 6, 1, 7)]


def on_device(orbitals, occupation, cutoff):
    axes = ("band", "grid")
    g = lax.axis_index("grid")
    core = lax.axis_index("band") % 2
    z, y = g % 8, g // 8
    y1 = y.reshape(1)
    give = lax.dynamic_slice(orbitals, (2 * (1 - y), 0, 0), (2, 3, ROW))
    came = ring(give, "grid", partner)
    blk = small_call(pack_body, [f32(24, HALF)], y1, orbitals, came, scalars=1)

    got = gather_blocks(blk)
    own, *lone = small_call(assemble_body, [f32(2, G, ROW), f32(G, ROW), f32(G, ROW)], *got)
    first = lax.ppermute(lone[0], axes, visit_route(0))
    twin = ring(own, "band", twin_of)

    late = lax.optimization_barrier((occupation, own))[0]
    weights = late.astype(jnp.float32) * -0.5
    w_own = lax.dynamic_slice(weights, (2 * y,), (2,))
    w_twin = ring(w_own, "band", twin_of)
    w_first = lax.ppermute(w_own[:1], axes, visit_route(0))
    held, w_held, first = lax.optimization_barrier((lone[1], w_own[1:], first))
    second = lax.ppermute(held, axes, visit_route(1))
    w_second = lax.ppermute(w_held, axes, visit_route(1))

    e = z * 2 + core
    once = [z == ORDER[v].index(7) for v in range(2)]
    idx = jnp.stack([e // 4 ^ 2 * core, e % 4 ^ 2 * core] + [o.astype(jnp.int32) for o in once])
    r = jnp.arange(G, dtype=jnp.int32)
    turned = basis(3 * (r // 3 % 2 * 8 + (z + r // 6) % 8) + r % 3)
    plain = jnp.asarray(plain_basis())
    tables = (kernel_table(cutoff), stacked(turned), stacked(turned.T), stacked(plain), stacked(plain.T))
    home, away, back = pair_solver(True, idx, w_own, w_twin, w_first, own, twin, first, *tables)
    ret0 = returned(back, 0)
    home, away, back = pair_solver(False, idx, w_own, w_twin, w_second, own, twin, second, *tables, home, away)
    ret1 = returned(back, 1)
    swapped = ring(away, "band", twin_of)
    part = small_call(disperse_body, [f32(24, HALF)] * 8, home, swapped, ret0, ret1)
    keep, give = small_call(unpack_body, [f32(2, 3, ROW)] * 2, y1, *scatter_blocks(part), scalars=1)
    came = ring(give, "grid", partner)
    return jnp.concatenate([jnp.where(y == 0, keep, came), jnp.where(y == 0, came, keep)], axis=0)


def solution(mesh):
    placed = (P("band", "grid", None), P("band"), P())
    return jax.shard_map(
        on_device, mesh=mesh, in_specs=placed, out_specs=P("band", "grid", None), check_vma=False
    )
```

```python
import functools

import numpy as np
import jax
import jax.numpy as jnp
from jax import lax
from jax.experimental import pallas as pl
from jax.experimental.pallas import tpu as pltpu
from jax.sharding import PartitionSpec as P


G = 48
ROW = G * G
HALF = ROW // 2
WITH_W = ROW + 128
WIDE = 256
YB = 8
LB = YB * G
VM = pl.BlockSpec(memory_space=pltpu.VMEM)
SM = pl.BlockSpec(memory_space=pltpu.SMEM)


def split2(x):
    hi = x.astype(jnp.bfloat16)
    lo = (x - hi.astype(jnp.float32)).astype(jnp.bfloat16)
    return jnp.concatenate([hi, lo], axis=0)


def apply(mat, x):
    both = jnp.dot(mat, split2(x), preferred_element_type=jnp.float32)
    return both[:G] + both[G:]


def f32(*shape):
    return jax.ShapeDtypeStruct(shape, jnp.float32)


def small_call(body, outs, *args, scalars=0):
    many = len(outs) > 1
    return pl.pallas_call(
        body,
        out_shape=outs if many else outs[0],
        in_specs=[SM] * scalars + [VM] * (len(args) - scalars),
        out_specs=[VM] * len(outs) if many else VM,
        compiler_params=pltpu.CompilerParams(vmem_limit_bytes=8 << 20),
        cost_estimate=pl.CostEstimate(flops=10**6, bytes_accessed=10**6, transcendentals=0),
    )(*args)


def pack_body(y, slab, came, blk):
    flip = y[0] != 0
    for o in range(2):
        mine = slab[2 * y[0] + o]
        other = came[o]
        a = jnp.where(flip, other, mine)
        b = jnp.where(flip, mine, other)
        for h in range(2):
            r = o * 12 + h * 6
            blk[r:r + 3, :] = a[:, h * HALF:(h + 1) * HALF]
            blk[r + 3:r + 6, :] = b[:, h * HALF:(h + 1) * HALF]


def assemble_body(y, occupation, *refs):
    both, lone = refs[8], refs[9:]
    for o in range(2):
        w = jnp.full((G, 128), occupation[2 * y[0] + o].astype(jnp.float32) * -0.5, jnp.float32)
        both[o, :, ROW:] = w
        lone[o][:, ROW:] = w
    for k in range(8):
        for o in range(2):
            for h in range(2):
                r = o * 12 + h * 6
                rows, lanes = slice(6 * k, 6 * k + 6), slice(h * HALF, (h + 1) * HALF)
                piece = refs[k][r:r + 6, :]
                both[o, rows, lanes] = piece
                lone[o][rows, lanes] = piece


def disperse_body(a, b, c0, c1, *outs):
    back = (c0, c1)
    for k in range(8):
        for o in range(2):
            for h in range(2):
                r = o * 12 + h * 6
                rows, lanes = slice(6 * k, 6 * k + 6), slice(h * HALF, (h + 1) * HALF)
                outs[k][r:r + 6, :] = a[o, rows, lanes] + b[o, rows, lanes] + back[o][rows, lanes]


def unpack_body(y, *refs):
    keep, give = refs[8:]
    flip = y[0] != 0
    for o in range(2):
        for h in range(2):
            r = o * 12 + h * 6
            total = refs[0][r:r + 6, :]
            for k in range(1, 8):
                total = total + refs[k][r:r + 6, :]
            a, b = total[:3], total[3:]
            keep[o, :, h * HALF:(h + 1) * HALF] = jnp.where(flip, b, a)
            give[o, :, h * HALF:(h + 1) * HALF] = jnp.where(flip, a, b)


def kernel(first, idx, own, twin, vis, ktab, fx, ix, fz, iz, *refs):
    prior = () if first else refs[:2]
    home, away, back, spec, *bufs = refs[len(prior):]
    gi, gj = idx[0], idx[1]
    once = idx[2] if first else idx[3]
    slots = 5 if first else 4

    def pick(i, lanes):
        return jnp.where(i < 2, own[i & 1, :, lanes], twin[i & 1, :, lanes])

    def ours(i, lanes):
        return own[i, :, lanes] if i < 2 else twin[i - 2, :, lanes]

    def enter_one(yb, rows, cols, zed):
        lanes = pl.ds(pl.multiple_of(yb * LB, LB), LB)
        for p in range(slots):
            r = ours(p, lanes) * vis[:, lanes] if p < 4 else pick(gi, lanes) * pick(gj, lanes)
            rows[p * G:(p + 1) * G, :] = apply(fx[...], r)
        for c in range(3):
            cols[c * 128:(c + 1) * 128, :] = rows[:, c * 128:(c + 1) * 128].T
        for y in range(YB):
            zed[y] = apply(fz[...], cols[y * G:(y + 1) * G, :])
        spec[:, pl.ds(pl.multiple_of(yb * YB, YB), YB), :] = jnp.swapaxes(zed[...], 0, 1)

    def enter(k, _):
        for u in range(3):
            enter_one(k * 3 + u, *bufs[u % 2 * 3:u % 2 * 3 + 3])
        return 0

    lax.fori_loop(0, G // YB // 3, enter, 0)

    def half_in(kz):
        return apply(fz[...], spec[kz]) * ktab[kz]

    for u in range(12):
        bufs[-1][u] = half_in(u)

    def middle(k, _):
        done = [apply(iz[...], bufs[-1][u]) for u in range(12)]
        for u in range(12):
            bufs[-1][u] = half_in((k + 1) * 12 + u)
        for u in range(12):
            spec[k * 12 + u] = done[u]
        return 0

    lax.fori_loop(0, G // 12 - 1, middle, 0)
    for u in range(12):
        spec[G - 12 + u] = apply(iz[...], bufs[-1][u])

    def spread(w):
        return jnp.concatenate([w] * (LB // 128), axis=1)

    keep = jnp.where(once != 0, 0.0, 1.0)
    tail = slice(ROW, WITH_W)
    wo = [spread((own if i < 2 else twin)[i % 2, 0:1, tail] * keep) for i in range(4)]
    wv = spread(vis[0:1, tail])
    if first:
        wj = spread(jnp.where(gj < 2, own[gj & 1, 0:1, tail], twin[gj & 1, 0:1, tail]))
        wg = jnp.where(gi < 2, wj, 0.0)
        wt = jnp.where(gi < 2, 0.0, wj)

    def leave_one(yb, rows, cols, zed):
        lanes = pl.ds(pl.multiple_of(yb * LB, LB), LB)
        zed[...] = jnp.swapaxes(spec[:, pl.ds(pl.multiple_of(yb * YB, YB), YB), :], 0, 1)
        for y in range(YB):
            cols[y * G:(y + 1) * G, :] = apply(iz[...], zed[y])
        for c in range(3):
            rows[:, c * 128:(c + 1) * 128] = cols[c * 128:(c + 1) * 128, :].T
        total = None
        v = vis[:, lanes] * wv
        for i in range(4):
            p = apply(ix[...], rows[i * G:(i + 1) * G, :])
            side = i // 2
            term = v * p
            if not first:
                term = term + prior[side][i % 2, :, lanes]
            (home, away)[side][i % 2, :, lanes] = term
            o = ours(i, lanes) * wo[i] * p
            total = o if total is None else total + o
        back[:, lanes] = total
        if first:
            p = pick(gj, lanes) * apply(ix[...], rows[4 * G:5 * G, :])
            home[gi & 1, :, lanes] = home[gi & 1, :, lanes] + p * wg
            away[gi & 1, :, lanes] = away[gi & 1, :, lanes] + p * wt

    def leave(k, _):
        for u in range(3):
            leave_one(k * 3 + u, *bufs[u % 2 * 3:u % 2 * 3 + 3])
        return 0

    lax.fori_loop(0, G // YB // 3, leave, 0)


def pair_solver(first, *args):
    return pl.pallas_call(
        functools.partial(kernel, first),
        out_shape=[f32(2, G, ROW), f32(2, G, ROW), f32(G, ROW)],
        in_specs=[SM] + [VM] * (len(args) - 1),
        out_specs=[VM] * 3,
        scratch_shapes=[
            pltpu.VMEM((G, G, WIDE), jnp.float32),
        ] + [
            pltpu.VMEM((WIDE, LB), jnp.float32),
            pltpu.VMEM((LB, WIDE), jnp.float32),
            pltpu.VMEM((YB, G, WIDE), jnp.float32),
        ] * 2 + [pltpu.VMEM((12, G, WIDE), jnp.float32)],
        compiler_params=pltpu.CompilerParams(vmem_limit_bytes=24 << 20),
        cost_estimate=pl.CostEstimate(flops=5 * 10**9, bytes_accessed=10**7, transcendentals=0),
    )(*args)


def stacked(m):
    top = lax.reduce_precision(m, 8, 7)
    hi = top.astype(jnp.bfloat16)
    lo = (m - top).astype(jnp.bfloat16)
    return jnp.concatenate([jnp.concatenate([hi, hi], 1), jnp.concatenate([lo, jnp.zeros_like(lo)], 1)], 0)


def plain_basis():
    k = np.arange(G)
    m = np.where(k <= G // 2, k, k - G // 2)
    ang = (2.0 * np.pi / G) * (m[:, None] * k[None, :] % G)
    return np.where((k <= G // 2)[:, None], np.cos(ang), np.sin(ang)).astype(np.float32)


def basis(place):
    k = jnp.arange(G, dtype=jnp.int32)
    m = jnp.where(k <= G // 2, k, k - G // 2)
    ang = (2.0 * np.pi / G) * ((m[:, None] * place[None, :]) % G).astype(jnp.float32)
    return jnp.where((k <= G // 2)[:, None], jnp.cos(ang), jnp.sin(ang))


def kernel_table(cutoff):
    def freq(shape, dim):
        k = lax.broadcasted_iota(jnp.int32, shape, dim) % G
        m = jnp.where(k <= G // 2, k, k - G // 2)
        return m * m, jnp.where((k == 0) | (k == G // 2), 1.0, 2.0)

    (a, wa), (b, wb), (c, wc) = freq((G, 1, 1), 0), freq((1, G, 1), 1), freq((1, 1, WIDE), 2)
    n = a + b + c
    ratios = n.astype(jnp.float32) * 0.5
    screen = jnp.where(n > 0, (1.0 - jnp.exp(-ratios)) / jnp.maximum(ratios, 0.5), 1.0)
    return jnp.where(n <= cutoff, 4.0 * screen * (wa * wb * wc / float(G**3)), 0.0)


def ring(block, axis, source):
    return lax.ppermute(block, axis, [(source(i), i) for i in range(lax.axis_size(axis))])


def partner(i):
    return (i + 8) % 16


def along(k):
    return lambda i: i // 8 * 8 + (i + k) % 8


def twin_of(i):
    return i ^ 1


OFFSETS = ((1, 0), (0, 1), (1, 1), (1, 3), (2, 1), (3, 2), None, (2, 0))
ORDER = ((2, 4, 6, 7, 0, 1, 3, 5), (0, 1, 3, 5, 2, 4, 6, 7))
MATCH = (5, 3, 2, 1, 4, 0, 6, 7)


def class_of(core, z, v):
    kind = ORDER[v][z]
    return MATCH[kind] if core else kind


def source_chip(kind, x, y):
    if kind == 6:
        px, py = x // 2, y // 2
        px, py = {(0, 0): (0, 1), (0, 1): (1, 0), (1, 0): (1, 1), (1, 1): (0, 0)}[(px, py)]
        return px * 2 + x % 2, py * 2 + y % 2
    dx, dy = OFFSETS[kind]
    return (x + dx) % 4, (y + dy) % 4


def visit_route(v, both_ways=True):
    pairs = []
    for b in range(16):
        for g in range(16):
            core, z = b % 2, g % 8
            kind = class_of(core, z, v)
            x, y = source_chip(kind, b // 2 % 4, g // 8 * 2 + b // 8)
            if both_ways or kind != 7:
                pairs.append(((((y % 2) * 4 + x) * 2 + core) * 16 + y // 2 * 8 + z, b * 16 + g))
    return pairs


def returned(back, v):
    return lax.ppermute(back, ("band", "grid"), [(d, s) for s, d in visit_route(v, False)])


def gather_blocks(b0):
    got = {0: b0}
    for k, source, hop in (
        (2, 0, 2), (6, 0, 6), (1, 0, 1), (7, 0, 7),
        (3, 2, 1), (5, 6, 7), (4, 2, 2),
    ):
        got[k] = ring(got[source], "grid", along(hop))
    return [got[k] for k in range(8)]


def scatter_blocks(part):
    return [part[0]] + [ring(part[k], "grid", along(-k)) for k in (4, 3, 5, 2, 6, 1, 7)]


def on_device(orbitals, occupation, cutoff):
    axes = ("band", "grid")
    g = lax.axis_index("grid")
    core = lax.axis_index("band") % 2
    z, y = g % 8, g // 8
    y1 = y.reshape(1)
    give = lax.dynamic_slice(orbitals, (2 * (1 - y), 0, 0), (2, 3, ROW))
    came = ring(give, "grid", partner)
    blk = small_call(pack_body, [f32(24, HALF)], y1, orbitals, came, scalars=1)

    got = gather_blocks(blk)
    e = z * 2 + core
    once = [z == ORDER[v].index(7) for v in range(2)]
    idx = jnp.stack([e // 4 ^ 2 * core, e % 4 ^ 2 * core] + [o.astype(jnp.int32) for o in once])
    r = jnp.arange(G, dtype=jnp.int32)
    turned = basis(3 * (r // 3 % 2 * 8 + (z + r // 6) % 8) + r % 3)
    plain = jnp.asarray(plain_basis())
    tables = (kernel_table(cutoff), stacked(turned), stacked(turned.T), stacked(plain), stacked(plain.T))
    got, idx, tables = lax.optimization_barrier((got, idx, tables))
    own, *lone = small_call(
        assemble_body, [f32(2, G, WITH_W), f32(G, WITH_W), f32(G, WITH_W)], y1, occupation, *got, scalars=2
    )
    vis0 = lax.ppermute(lone[0], axes, visit_route(0))
    twin = ring(own, "band", twin_of)
    held, vis0 = lax.optimization_barrier((lone[1], vis0))
    vis1 = lax.ppermute(held, axes, visit_route(1))

    home, away, back = pair_solver(True, idx, own, twin, vis0, *tables)
    ret0 = returned(back, 0)
    home, away, back = pair_solver(False, idx, own, twin, vis1, *tables, home, away)
    ret1 = returned(back, 1)
    swapped = ring(away, "band", twin_of)
    part = small_call(disperse_body, [f32(24, HALF)] * 8, home, swapped, ret0, ret1)
    keep, give = small_call(unpack_body, [f32(2, 3, ROW)] * 2, y1, *scatter_blocks(part), scalars=1)
    came = ring(give, "grid", partner)
    return jnp.concatenate([jnp.where(y == 0, keep, came), jnp.where(y == 0, came, keep)], axis=0)


def solution(mesh):
    placed = (P("band", "grid", None), P("band"), P())
    return jax.shard_map(
        on_device, mesh=mesh, in_specs=placed, out_specs=P("band", "grid", None), check_vma=False
    )
```

```python
import functools

import numpy as np
import jax
import jax.numpy as jnp
from jax import lax
from jax.experimental import pallas as pl
from jax.experimental.pallas import tpu as pltpu
from jax.sharding import PartitionSpec as P


G = 48
ROW = G * G
HALF = ROW // 2
WITH_W = ROW + 128
WIDE = 256
YB = 8
LB = YB * G
VM = pl.BlockSpec(memory_space=pltpu.VMEM)
SM = pl.BlockSpec(memory_space=pltpu.SMEM)


def split2(x):
    hi = x.astype(jnp.bfloat16)
    lo = (x - hi.astype(jnp.float32)).astype(jnp.bfloat16)
    return jnp.concatenate([hi, lo], axis=0)


def apply(mat, x):
    both = jnp.dot(mat, split2(x), preferred_element_type=jnp.float32)
    return both[:G] + both[G:]


def f32(*shape):
    return jax.ShapeDtypeStruct(shape, jnp.float32)


def small_call(body, outs, *args, scalars=0):
    many = len(outs) > 1
    return pl.pallas_call(
        body,
        out_shape=outs if many else outs[0],
        in_specs=[SM] * scalars + [VM] * (len(args) - scalars),
        out_specs=[VM] * len(outs) if many else VM,
        compiler_params=pltpu.CompilerParams(vmem_limit_bytes=8 << 20),
        cost_estimate=pl.CostEstimate(flops=10**6, bytes_accessed=10**6, transcendentals=0),
    )(*args)


def pack_body(y, slab, came, blk):
    flip = y[0] != 0
    for o in range(2):
        mine = slab[2 * y[0] + o]
        other = came[o]
        a = jnp.where(flip, other, mine)
        b = jnp.where(flip, mine, other)
        for h in range(2):
            r = o * 12 + h * 6
            blk[r:r + 3, :] = a[:, h * HALF:(h + 1) * HALF]
            blk[r + 3:r + 6, :] = b[:, h * HALF:(h + 1) * HALF]


def assemble_body(y, occupation, *refs):
    both, lone = refs[8], refs[9:]
    for o in range(2):
        w = jnp.full((G, 128), occupation[2 * y[0] + o].astype(jnp.float32) * -0.5, jnp.float32)
        both[o, :, ROW:] = w
        lone[o][:, ROW:] = w
    for k in range(8):
        for o in range(2):
            for h in range(2):
                r = o * 12 + h * 6
                rows, lanes = slice(6 * k, 6 * k + 6), slice(h * HALF, (h + 1) * HALF)
                piece = refs[k][r:r + 6, :]
                both[o, rows, lanes] = piece
                lone[o][rows, lanes] = piece


def disperse_body(a, b, c0, c1, own, up1, up2, down1, down2, far_up, far_down):
    back = (c0, c1)
    near = {0: own, 1: up1, 2: up2, 7: down1, 6: down2}
    for k in range(8):
        for o in range(2):
            for h in range(2):
                r = o * 12 + h * 6
                rows, lanes = slice(6 * k, 6 * k + 6), slice(h * HALF, (h + 1) * HALF)
                total = a[o, rows, lanes] + b[o, rows, lanes] + back[o][rows, lanes]
                if k in near:
                    near[k][r:r + 6, :] = total
                elif k != 4:
                    (far_up if k == 3 else far_down)[r:r + 6, :] = total
                else:
                    (far_down if o else far_up)[24 + h * 6:30 + h * 6, :] = total


def merge_body(up1, up2, down1, down2, far_up, far_down, to_up1, to_up2, to_down1, to_down2):
    to_up1[...] = up1[...] + far_up[:24, :]
    to_down1[...] = down1[...] + far_down[:24, :]
    to_up2[:12, :] = up2[:12, :] + far_up[24:, :]
    to_up2[12:, :] = up2[12:, :]
    to_down2[:12, :] = down2[:12, :]
    to_down2[12:, :] = down2[12:, :] + far_down[24:, :]


def unpack_body(y, *refs):
    keep, give = refs[5:]
    flip = y[0] != 0
    for o in range(2):
        for h in range(2):
            r = o * 12 + h * 6
            total = refs[0][r:r + 6, :]
            for k in range(1, 5):
                total = total + refs[k][r:r + 6, :]
            a, b = total[:3], total[3:]
            keep[o, :, h * HALF:(h + 1) * HALF] = jnp.where(flip, b, a)
            give[o, :, h * HALF:(h + 1) * HALF] = jnp.where(flip, a, b)


def kernel(first, idx, own, twin, vis, ktab, fx, ix, fz, iz, *refs):
    prior = () if first else refs[:2]
    home, away, back, spec, *bufs = refs[len(prior):]
    gi, gj = idx[0], idx[1]
    once = idx[2] if first else idx[3]
    slots = 5 if first else 4

    def pick(i, lanes):
        return jnp.where(i < 2, own[i & 1, :, lanes], twin[i & 1, :, lanes])

    def ours(i, lanes):
        return own[i, :, lanes] if i < 2 else twin[i - 2, :, lanes]

    def enter_one(yb, rows, cols, zed):
        lanes = pl.ds(pl.multiple_of(yb * LB, LB), LB)
        for p in range(slots):
            r = ours(p, lanes) * vis[:, lanes] if p < 4 else pick(gi, lanes) * pick(gj, lanes)
            rows[p * G:(p + 1) * G, :] = apply(fx[...], r)
        for c in range(3):
            cols[c * 128:(c + 1) * 128, :] = rows[:, c * 128:(c + 1) * 128].T
        for y in range(YB):
            zed[y] = apply(fz[...], cols[y * G:(y + 1) * G, :])
        spec[:, pl.ds(pl.multiple_of(yb * YB, YB), YB), :] = jnp.swapaxes(zed[...], 0, 1)

    def enter(k, _):
        for u in range(6):
            enter_one(k * 6 + u, *bufs[u % 2 * 3:u % 2 * 3 + 3])
        return 0

    lax.fori_loop(0, G // YB // 6, enter, 0)

    def half_in(kz):
        return apply(fz[...], spec[kz]) * ktab[kz]

    for u in range(12):
        bufs[-1][u] = half_in(u)

    def middle(k, _):
        done = [apply(iz[...], bufs[-1][u]) for u in range(12)]
        for u in range(12):
            bufs[-1][u] = half_in((k + 1) * 12 + u)
        for u in range(12):
            spec[k * 12 + u] = done[u]
        return 0

    lax.fori_loop(0, G // 12 - 1, middle, 0)
    for u in range(12):
        spec[G - 12 + u] = apply(iz[...], bufs[-1][u])

    def spread(w):
        return jnp.concatenate([w] * (LB // 128), axis=1)

    keep = jnp.where(once != 0, 0.0, 1.0)
    tail = slice(ROW, WITH_W)
    wo = [spread((own if i < 2 else twin)[i % 2, 0:1, tail] * keep) for i in range(4)]
    wv = spread(vis[0:1, tail])
    if first:
        wj = spread(jnp.where(gj < 2, own[gj & 1, 0:1, tail], twin[gj & 1, 0:1, tail]))
        wg = jnp.where(gi < 2, wj, 0.0)
        wt = jnp.where(gi < 2, 0.0, wj)

    def leave_one(yb, rows, cols, zed):
        lanes = pl.ds(pl.multiple_of(yb * LB, LB), LB)
        zed[...] = jnp.swapaxes(spec[:, pl.ds(pl.multiple_of(yb * YB, YB), YB), :], 0, 1)
        for y in range(YB):
            cols[y * G:(y + 1) * G, :] = apply(iz[...], zed[y])
        for c in range(3):
            rows[:, c * 128:(c + 1) * 128] = cols[c * 128:(c + 1) * 128, :].T
        total = None
        v = vis[:, lanes] * wv
        for i in range(4):
            p = apply(ix[...], rows[i * G:(i + 1) * G, :])
            side = i // 2
            term = v * p
            if not first:
                term = term + prior[side][i % 2, :, lanes]
            (home, away)[side][i % 2, :, lanes] = term
            o = ours(i, lanes) * wo[i] * p
            total = o if total is None else total + o
        back[:, lanes] = total
        if first:
            p = pick(gj, lanes) * apply(ix[...], rows[4 * G:5 * G, :])
            home[gi & 1, :, lanes] = home[gi & 1, :, lanes] + p * wg
            away[gi & 1, :, lanes] = away[gi & 1, :, lanes] + p * wt

    def leave(k, _):
        for u in range(6):
            leave_one(k * 6 + u, *bufs[u % 2 * 3:u % 2 * 3 + 3])
        return 0

    lax.fori_loop(0, G // YB // 6, leave, 0)


def pair_solver(first, *args):
    return pl.pallas_call(
        functools.partial(kernel, first),
        out_shape=[f32(2, G, ROW), f32(2, G, ROW), f32(G, ROW)],
        in_specs=[SM] + [VM] * (len(args) - 1),
        out_specs=[VM] * 3,
        scratch_shapes=[
            pltpu.VMEM((G, G, WIDE), jnp.float32),
        ] + [
            pltpu.VMEM((WIDE, LB), jnp.float32),
            pltpu.VMEM((LB, WIDE), jnp.float32),
            pltpu.VMEM((YB, G, WIDE), jnp.float32),
        ] * 2 + [pltpu.VMEM((12, G, WIDE), jnp.float32)],
        compiler_params=pltpu.CompilerParams(vmem_limit_bytes=24 << 20),
        cost_estimate=pl.CostEstimate(flops=5 * 10**9, bytes_accessed=10**7, transcendentals=0),
    )(*args)


def stacked(m):
    top = lax.reduce_precision(m, 8, 7)
    hi = top.astype(jnp.bfloat16)
    lo = (m - top).astype(jnp.bfloat16)
    return jnp.concatenate([jnp.concatenate([hi, hi], 1), jnp.concatenate([lo, jnp.zeros_like(lo)], 1)], 0)


def plain_basis():
    k = np.arange(G)
    m = np.where(k <= G // 2, k, k - G // 2)
    ang = (2.0 * np.pi / G) * (m[:, None] * k[None, :] % G)
    return np.where((k <= G // 2)[:, None], np.cos(ang), np.sin(ang)).astype(np.float32)


def basis(place):
    k = jnp.arange(G, dtype=jnp.int32)
    m = jnp.where(k <= G // 2, k, k - G // 2)
    ang = (2.0 * np.pi / G) * ((m[:, None] * place[None, :]) % G).astype(jnp.float32)
    return jnp.where((k <= G // 2)[:, None], jnp.cos(ang), jnp.sin(ang))


def kernel_table(cutoff):
    def freq(shape, dim):
        k = lax.broadcasted_iota(jnp.int32, shape, dim) % G
        m = jnp.where(k <= G // 2, k, k - G // 2)
        return m * m, jnp.where((k == 0) | (k == G // 2), 1.0, 2.0)

    (a, wa), (b, wb), (c, wc) = freq((G, 1, 1), 0), freq((1, G, 1), 1), freq((1, 1, WIDE), 2)
    n = a + b + c
    ratios = n.astype(jnp.float32) * 0.5
    screen = jnp.where(n > 0, (1.0 - jnp.exp(-ratios)) / jnp.maximum(ratios, 0.5), 1.0)
    return jnp.where(n <= cutoff, 4.0 * screen * (wa * wb * wc / float(G**3)), 0.0)


def ring(block, axis, source):
    return lax.ppermute(block, axis, [(source(i), i) for i in range(lax.axis_size(axis))])


def partner(i):
    return (i + 8) % 16


def along(k):
    return lambda i: i // 8 * 8 + (i + k) % 8


def twin_of(i):
    return i ^ 1


OFFSETS = ((1, 0), (0, 1), (1, 1), (1, 3), (2, 1), (3, 2), None, (2, 0))
ORDER = ((2, 4, 6, 7, 0, 1, 3, 5), (0, 1, 3, 5, 2, 4, 6, 7))
MATCH = (5, 3, 2, 1, 4, 0, 6, 7)


def class_of(core, z, v):
    kind = ORDER[v][z]
    return MATCH[kind] if core else kind


def source_chip(kind, x, y):
    if kind == 6:
        px, py = x // 2, y // 2
        px, py = {(0, 0): (0, 1), (0, 1): (1, 0), (1, 0): (1, 1), (1, 1): (0, 0)}[(px, py)]
        return px * 2 + x % 2, py * 2 + y % 2
    dx, dy = OFFSETS[kind]
    return (x + dx) % 4, (y + dy) % 4


def visit_route(v, both_ways=True):
    pairs = []
    for b in range(16):
        for g in range(16):
            core, z = b % 2, g % 8
            kind = class_of(core, z, v)
            x, y = source_chip(kind, b // 2 % 4, g // 8 * 2 + b // 8)
            if both_ways or kind != 7:
                pairs.append(((((y % 2) * 4 + x) * 2 + core) * 16 + y // 2 * 8 + z, b * 16 + g))
    return pairs


def returned(back, v):
    return lax.ppermute(back, ("band", "grid"), [(d, s) for s, d in visit_route(v, False)])


def gather_blocks(b0):
    got = {0: b0}
    for k, source, hop in (
        (2, 0, 2), (6, 0, 6), (1, 0, 1), (7, 0, 7),
        (3, 2, 1), (5, 6, 7), (4, 2, 2),
    ):
        got[k] = ring(got[source], "grid", along(hop))
    return [got[k] for k in range(8)]


def scatter_blocks(own, up1, up2, down1, down2, far_up, far_down):
    far_up = ring(far_up, "grid", along(-2))
    far_down = ring(far_down, "grid", along(2))
    up1, up2, down1, down2 = small_call(
        merge_body, [f32(24, HALF)] * 4, up1, up2, down1, down2, far_up, far_down
    )
    hops = ((up2, -2), (down2, 2), (up1, -1), (down1, 1))
    return [own] + [ring(block, "grid", along(hop)) for block, hop in hops]


def on_device(orbitals, occupation, cutoff):
    axes = ("band", "grid")
    g = lax.axis_index("grid")
    core = lax.axis_index("band") % 2
    z, y = g % 8, g // 8
    y1 = y.reshape(1)
    give = lax.dynamic_slice(orbitals, (2 * (1 - y), 0, 0), (2, 3, ROW))
    came = ring(give, "grid", partner)
    blk = small_call(pack_body, [f32(24, HALF)], y1, orbitals, came, scalars=1)

    got = gather_blocks(blk)
    e = z * 2 + core
    once = [z == ORDER[v].index(7) for v in range(2)]
    idx = jnp.stack([e // 4 ^ 2 * core, e % 4 ^ 2 * core] + [o.astype(jnp.int32) for o in once])
    r = jnp.arange(G, dtype=jnp.int32)
    turned = basis(3 * (r // 3 % 2 * 8 + (z + r // 6) % 8) + r % 3)
    plain = jnp.asarray(plain_basis())
    tables = (kernel_table(cutoff), stacked(turned), stacked(turned.T), stacked(plain), stacked(plain.T))
    got, idx, tables = lax.optimization_barrier((got, idx, tables))
    own, *lone = small_call(
        assemble_body, [f32(2, G, WITH_W), f32(G, WITH_W), f32(G, WITH_W)], y1, occupation, *got, scalars=2
    )
    vis0 = lax.ppermute(lone[0], axes, visit_route(0))
    twin = ring(own, "band", twin_of)
    held, vis0 = lax.optimization_barrier((lone[1], vis0))
    vis1 = lax.ppermute(held, axes, visit_route(1))

    home, away, back = pair_solver(True, idx, own, twin, vis0, *tables)
    ret0 = returned(back, 0)
    home, away, back = pair_solver(False, idx, own, twin, vis1, *tables, home, away)
    ret1 = returned(back, 1)
    swapped = ring(away, "band", twin_of)
    part = small_call(disperse_body, [f32(24, HALF)] * 5 + [f32(36, HALF)] * 2, home, swapped, ret0, ret1)
    keep, give = small_call(unpack_body, [f32(2, 3, ROW)] * 2, y1, *scatter_blocks(*part), scalars=1)
    came = ring(give, "grid", partner)
    return jnp.concatenate([jnp.where(y == 0, keep, came), jnp.where(y == 0, came, keep)], axis=0)


def solution(mesh):
    placed = (P("band", "grid", None), P("band"), P())
    return jax.shard_map(
        on_device, mesh=mesh, in_specs=placed, out_specs=P("band", "grid", None), check_vma=False
    )
```

```python
import functools

import numpy as np
import jax
import jax.numpy as jnp
from jax import lax
from jax.experimental import pallas as pl
from jax.experimental.pallas import tpu as pltpu
from jax.sharding import PartitionSpec as P


G = 48
ROW = G * G
HALF = ROW // 2
WITH_W = ROW + 128
WIDE = 256
YB = 8
LB = YB * G
VM = pl.BlockSpec(memory_space=pltpu.VMEM)
SM = pl.BlockSpec(memory_space=pltpu.SMEM)


def split2(x):
    hi = x.astype(jnp.bfloat16)
    lo = (x - hi.astype(jnp.float32)).astype(jnp.bfloat16)
    return jnp.concatenate([hi, lo], axis=0)


def apply(mat, x):
    both = jnp.dot(mat, split2(x), preferred_element_type=jnp.float32)
    return both[:G] + both[G:]


def f32(*shape):
    return jax.ShapeDtypeStruct(shape, jnp.float32)


def small_call(body, outs, *args, scalars=0):
    many = len(outs) > 1
    return pl.pallas_call(
        body,
        out_shape=outs if many else outs[0],
        in_specs=[SM] * scalars + [VM] * (len(args) - scalars),
        out_specs=[VM] * len(outs) if many else VM,
        compiler_params=pltpu.CompilerParams(vmem_limit_bytes=8 << 20),
        cost_estimate=pl.CostEstimate(flops=10**6, bytes_accessed=10**6, transcendentals=0),
    )(*args)


def pack_body(y, slab, came, blk):
    flip = y[0] != 0
    for o in range(2):
        for x in range(3):
            mine = jnp.where(flip, slab[x, o + 2:o + 3, :], slab[x, o:o + 1, :])
            other = came[x, o:o + 1, :]
            a = jnp.where(flip, other, mine)
            b = jnp.where(flip, mine, other)
            for h in range(2):
                r = o * 12 + h * 6 + x
                blk[r:r + 1, :] = a[:, h * HALF:(h + 1) * HALF]
                blk[r + 3:r + 4, :] = b[:, h * HALF:(h + 1) * HALF]


def assemble_body(y, occupation, *refs):
    both, lone = refs[8], refs[9:]
    for o in range(2):
        w = jnp.full((G, 128), occupation[2 * y[0] + o].astype(jnp.float32) * -0.5, jnp.float32)
        both[o, :, ROW:] = w
        lone[o][:, ROW:] = w
    for k in range(8):
        for o in range(2):
            for h in range(2):
                r = o * 12 + h * 6
                rows, lanes = slice(6 * k, 6 * k + 6), slice(h * HALF, (h + 1) * HALF)
                piece = refs[k][r:r + 6, :]
                both[o, rows, lanes] = piece
                lone[o][rows, lanes] = piece


def disperse_body(a, b, c0, c1, *outs):
    back = (c0, c1)
    for k in range(8):
        for o in range(2):
            for h in range(2):
                r = o * 12 + h * 6
                rows, lanes = slice(6 * k, 6 * k + 6), slice(h * HALF, (h + 1) * HALF)
                outs[k][r:r + 6, :] = a[o, rows, lanes] + b[o, rows, lanes] + back[o][rows, lanes]


def merge_body(core, up2, down2, far, to_up2, to_down2):
    moved = far[...]
    to_up2[...] = up2[...] + jnp.where(core[0] == 0, moved, 0.0)
    to_down2[...] = down2[...] + jnp.where(core[0] == 0, 0.0, moved)


def unpack_body(y, *refs):
    keep, give = refs[7:]
    flip = y[0] != 0
    for o in range(2):
        for h in range(2):
            r = o * 12 + h * 6
            total = refs[0][r:r + 6, :]
            for k in range(1, 7):
                total = total + refs[k][r:r + 6, :]
            for x in range(3):
                a, b = total[x:x + 1], total[x + 3:x + 4]
                keep[x, o:o + 1, h * HALF:(h + 1) * HALF] = jnp.where(flip, b, a)
                give[x, o:o + 1, h * HALF:(h + 1) * HALF] = jnp.where(flip, a, b)


def kernel(first, idx, own, twin, vis, ktab, fx, ix, fz, iz, *refs):
    prior = () if first else refs[:2]
    home, away, back, spec, *bufs = refs[len(prior):]
    gi, gj = idx[0], idx[1]
    once = idx[2] if first else idx[3]
    slots = 5 if first else 4

    def pick(i, lanes):
        return jnp.where(i < 2, own[i & 1, :, lanes], twin[i & 1, :, lanes])

    def ours(i, lanes):
        return own[i, :, lanes] if i < 2 else twin[i - 2, :, lanes]

    def enter_one(yb, rows, cols, zed):
        lanes = pl.ds(pl.multiple_of(yb * LB, LB), LB)
        for p in range(slots):
            r = ours(p, lanes) * vis[:, lanes] if p < 4 else pick(gi, lanes) * pick(gj, lanes)
            rows[p * G:(p + 1) * G, :] = apply(fx[...], r)
        for c in range(3):
            cols[c * 128:(c + 1) * 128, :] = rows[:, c * 128:(c + 1) * 128].T
        for y in range(YB):
            zed[y] = apply(fz[...], cols[y * G:(y + 1) * G, :])
        spec[:, pl.ds(pl.multiple_of(yb * YB, YB), YB), :] = jnp.swapaxes(zed[...], 0, 1)

    def enter(k, _):
        for u in range(6):
            enter_one(k * 6 + u, *bufs[u % 2 * 3:u % 2 * 3 + 3])
        return 0

    lax.fori_loop(0, G // YB // 6, enter, 0)

    def half_in(kz):
        return apply(fz[...], spec[kz]) * ktab[kz]

    for u in range(12):
        bufs[-1][u] = half_in(u)

    def middle(k, _):
        done = [apply(iz[...], bufs[-1][u]) for u in range(12)]
        for u in range(12):
            bufs[-1][u] = half_in((k + 1) * 12 + u)
        for u in range(12):
            spec[k * 12 + u] = done[u]
        return 0

    lax.fori_loop(0, G // 12 - 1, middle, 0)
    for u in range(12):
        spec[G - 12 + u] = apply(iz[...], bufs[-1][u])

    def spread(w):
        return jnp.concatenate([w] * (LB // 128), axis=1)

    keep = jnp.where(once != 0, 0.0, 1.0)
    tail = slice(ROW, WITH_W)
    wo = [spread((own if i < 2 else twin)[i % 2, 0:1, tail] * keep) for i in range(4)]
    wv = spread(vis[0:1, tail])
    if first:
        wj = spread(jnp.where(gj < 2, own[gj & 1, 0:1, tail], twin[gj & 1, 0:1, tail]))
        wg = jnp.where(gi < 2, wj, 0.0)
        wt = jnp.where(gi < 2, 0.0, wj)

    def leave_one(yb, rows, cols, zed):
        lanes = pl.ds(pl.multiple_of(yb * LB, LB), LB)
        zed[...] = jnp.swapaxes(spec[:, pl.ds(pl.multiple_of(yb * YB, YB), YB), :], 0, 1)
        for y in range(YB):
            cols[y * G:(y + 1) * G, :] = apply(iz[...], zed[y])
        for c in range(3):
            rows[:, c * 128:(c + 1) * 128] = cols[c * 128:(c + 1) * 128, :].T
        total = None
        v = vis[:, lanes] * wv
        for i in range(4):
            p = apply(ix[...], rows[i * G:(i + 1) * G, :])
            side = i // 2
            term = v * p
            if not first:
                term = term + prior[side][i % 2, :, lanes]
            (home, away)[side][i % 2, :, lanes] = term
            o = ours(i, lanes) * wo[i] * p
            total = o if total is None else total + o
        back[:, lanes] = total
        if first:
            p = pick(gj, lanes) * apply(ix[...], rows[4 * G:5 * G, :])
            home[gi & 1, :, lanes] = home[gi & 1, :, lanes] + p * wg
            away[gi & 1, :, lanes] = away[gi & 1, :, lanes] + p * wt

    def leave(k, _):
        for u in range(6):
            leave_one(k * 6 + u, *bufs[u % 2 * 3:u % 2 * 3 + 3])
        return 0

    lax.fori_loop(0, G // YB // 6, leave, 0)


def pair_solver(first, *args):
    return pl.pallas_call(
        functools.partial(kernel, first),
        out_shape=[f32(2, G, ROW), f32(2, G, ROW), f32(G, ROW)],
        in_specs=[SM] + [VM] * (len(args) - 1),
        out_specs=[VM] * 3,
        scratch_shapes=[
            pltpu.VMEM((G, G, WIDE), jnp.float32),
        ] + [
            pltpu.VMEM((WIDE, LB), jnp.float32),
            pltpu.VMEM((LB, WIDE), jnp.float32),
            pltpu.VMEM((YB, G, WIDE), jnp.float32),
        ] * 2 + [pltpu.VMEM((12, G, WIDE), jnp.float32)],
        compiler_params=pltpu.CompilerParams(vmem_limit_bytes=24 << 20),
        cost_estimate=pl.CostEstimate(flops=5 * 10**9, bytes_accessed=10**7, transcendentals=0),
    )(*args)


def stacked(m):
    top = lax.reduce_precision(m, 8, 7)
    hi = top.astype(jnp.bfloat16)
    lo = (m - top).astype(jnp.bfloat16)
    return jnp.concatenate([jnp.concatenate([hi, hi], 1), jnp.concatenate([lo, jnp.zeros_like(lo)], 1)], 0)


def plain_basis():
    k = np.arange(G)
    m = np.where(k <= G // 2, k, k - G // 2)
    ang = (2.0 * np.pi / G) * (m[:, None] * k[None, :] % G)
    return np.where((k <= G // 2)[:, None], np.cos(ang), np.sin(ang)).astype(np.float32)


def basis(place):
    k = jnp.arange(G, dtype=jnp.int32)
    m = jnp.where(k <= G // 2, k, k - G // 2)
    ang = (2.0 * np.pi / G) * ((m[:, None] * place[None, :]) % G).astype(jnp.float32)
    return jnp.where((k <= G // 2)[:, None], jnp.cos(ang), jnp.sin(ang))


def kernel_table(cutoff):
    def freq(shape, dim):
        k = lax.broadcasted_iota(jnp.int32, shape, dim) % G
        m = jnp.where(k <= G // 2, k, k - G // 2)
        return m * m, jnp.where((k == 0) | (k == G // 2), 1.0, 2.0)

    (a, wa), (b, wb), (c, wc) = freq((G, 1, 1), 0), freq((1, G, 1), 1), freq((1, 1, WIDE), 2)
    n = a + b + c
    ratios = n.astype(jnp.float32) * 0.5
    screen = jnp.where(n > 0, (1.0 - jnp.exp(-ratios)) / jnp.maximum(ratios, 0.5), 1.0)
    return jnp.where(n <= cutoff, 4.0 * screen * (wa * wb * wc / float(G**3)), 0.0)


def ring(block, axis, source):
    return lax.ppermute(block, axis, [(source(i), i) for i in range(lax.axis_size(axis))])


def partner(i):
    return (i + 8) % 16


def along(k):
    return lambda i: i // 8 * 8 + (i + k) % 8


def twin_of(i):
    return i ^ 1


OFFSETS = ((1, 0), (0, 1), (1, 1), (1, 3), (2, 1), (3, 2), None, (2, 0))
ORDER = ((2, 4, 6, 7, 0, 1, 3, 5), (0, 1, 3, 5, 2, 4, 6, 7))
MATCH = (5, 3, 2, 1, 4, 0, 6, 7)


def class_of(core, z, v):
    kind = ORDER[v][z]
    return MATCH[kind] if core else kind


def source_chip(kind, x, y):
    if kind == 6:
        px, py = x // 2, y // 2
        px, py = {(0, 0): (0, 1), (0, 1): (1, 0), (1, 0): (1, 1), (1, 1): (0, 0)}[(px, py)]
        return px * 2 + x % 2, py * 2 + y % 2
    dx, dy = OFFSETS[kind]
    return (x + dx) % 4, (y + dy) % 4


def visit_route(v, both_ways=True):
    pairs = []
    for b in range(16):
        for g in range(16):
            core, z = b % 2, g % 8
            kind = class_of(core, z, v)
            x, y = source_chip(kind, b // 2 % 4, g // 8 * 2 + b // 8)
            if both_ways or kind != 7:
                pairs.append(((((y % 2) * 4 + x) * 2 + core) * 16 + y // 2 * 8 + z, b * 16 + g))
    return pairs


def returned(back, v):
    return lax.ppermute(back, ("band", "grid"), [(d, s) for s, d in visit_route(v, False)])


def by_core(hop):
    return [
        (b * 16 + along(-hop if b % 2 else hop)(g), b * 16 + g) for b in range(16) for g in range(16)
    ]


def gather_blocks(b0, core):
    got = {0: b0}
    for k, source, hop in (
        (2, 0, 2), (6, 0, 6), (1, 0, 1), (7, 0, 7),
        (3, 2, 1), (5, 6, 7),
    ):
        got[k] = ring(got[source], "grid", along(hop))
    got[4] = lax.ppermute(jnp.where(core == 0, got[2], got[6]), ("band", "grid"), by_core(2))
    return [got[k] for k in range(8)]


def scatter_blocks(core, own, up1, up2, up3, far, down3, down2, down1):
    far = lax.ppermute(far, ("band", "grid"), by_core(-2))
    came = [own]
    for block, hop in ((up3, -3), (down3, 3), (up1, -1), (down1, 1)):
        came.append(ring(block, "grid", along(hop)))
    up2, down2 = small_call(
        merge_body, [f32(24, HALF)] * 2, core.reshape(1), up2, down2, far, scalars=1
    )
    return came + [ring(up2, "grid", along(-2)), ring(down2, "grid", along(2))]


def on_device(orbitals, occupation, cutoff):
    axes = ("band", "grid")
    g = lax.axis_index("grid")
    core = lax.axis_index("band") % 2
    z, y = g % 8, g // 8
    y1 = y.reshape(1)
    slab = orbitals.transpose(1, 0, 2)
    give = jnp.where(y == 0, slab[:, 2:], slab[:, :2])
    came = ring(give, "grid", partner)
    blk = small_call(pack_body, [f32(24, HALF)], y1, slab, came, scalars=1)

    got = gather_blocks(blk, core)
    e = z * 2 + core
    once = [z == ORDER[v].index(7) for v in range(2)]
    idx = jnp.stack([e // 4 ^ 2 * core, e % 4 ^ 2 * core] + [o.astype(jnp.int32) for o in once])
    r = jnp.arange(G, dtype=jnp.int32)
    turned = basis(3 * (r // 3 % 2 * 8 + (z + r // 6) % 8) + r % 3)
    plain = jnp.asarray(plain_basis())
    tables = (kernel_table(cutoff), stacked(turned), stacked(turned.T), stacked(plain), stacked(plain.T))
    got, idx, tables = lax.optimization_barrier((got, idx, tables))
    own, *lone = small_call(
        assemble_body, [f32(2, G, WITH_W), f32(G, WITH_W), f32(G, WITH_W)], y1, occupation, *got, scalars=2
    )
    vis0 = lax.ppermute(lone[0], axes, visit_route(0))
    twin = ring(own, "band", twin_of)
    held, vis0 = lax.optimization_barrier((lone[1], vis0))
    vis1 = lax.ppermute(held, axes, visit_route(1))

    home, away, back = pair_solver(True, idx, own, twin, vis0, *tables)
    ret0 = returned(back, 0)
    home, away, back = pair_solver(False, idx, own, twin, vis1, *tables, home, away)
    ret1 = returned(back, 1)
    swapped = ring(away, "band", twin_of)
    part = small_call(disperse_body, [f32(24, HALF)] * 8, home, swapped, ret0, ret1)
    keep, give = small_call(unpack_body, [f32(3, 2, ROW)] * 2, y1, *scatter_blocks(core, *part), scalars=1)
    came = ring(give, "grid", partner)
    out = jnp.concatenate([jnp.where(y == 0, keep, came), jnp.where(y == 0, came, keep)], axis=1)
    return out.transpose(1, 0, 2)


def solution(mesh):
    placed = (P("band", "grid", None), P("band"), P())
    return jax.shard_map(
        on_device, mesh=mesh, in_specs=placed, out_specs=P("band", "grid", None), check_vma=False
    )
```

```python
import functools

import numpy as np
import jax
import jax.numpy as jnp
from jax import lax
from jax.experimental import pallas as pl
from jax.experimental.pallas import tpu as pltpu
from jax.sharding import PartitionSpec as P


G = 48
ROW = G * G
HALF = ROW // 2
WITH_W = ROW + 128
WIDE = 256
YB = 8
LB = YB * G
VM = pl.BlockSpec(memory_space=pltpu.VMEM)
SM = pl.BlockSpec(memory_space=pltpu.SMEM)


def split2(x):
    hi = x.astype(jnp.bfloat16)
    lo = (x - hi.astype(jnp.float32)).astype(jnp.bfloat16)
    return jnp.concatenate([hi, lo], axis=0)


def apply(mat, x):
    both = jnp.dot(mat, split2(x), preferred_element_type=jnp.float32)
    return both[:G] + both[G:]


def f32(*shape):
    return jax.ShapeDtypeStruct(shape, jnp.float32)


def small_call(body, outs, *args, scalars=0):
    many = len(outs) > 1
    return pl.pallas_call(
        body,
        out_shape=outs if many else outs[0],
        in_specs=[SM] * scalars + [VM] * (len(args) - scalars),
        out_specs=[VM] * len(outs) if many else VM,
        compiler_params=pltpu.CompilerParams(vmem_limit_bytes=8 << 20),
        cost_estimate=pl.CostEstimate(flops=10**6, bytes_accessed=10**6, transcendentals=0),
    )(*args)


def pack_body(y, slab, came, blk):
    flip = y[0] != 0
    for o in range(2):
        for x in range(3):
            mine = jnp.where(flip, slab[x, o + 2:o + 3, :], slab[x, o:o + 1, :])
            other = came[x, o:o + 1, :]
            a = jnp.where(flip, other, mine)
            b = jnp.where(flip, mine, other)
            for h in range(2):
                r = o * 12 + h * 6 + x
                blk[r:r + 1, :] = a[:, h * HALF:(h + 1) * HALF]
                blk[r + 3:r + 4, :] = b[:, h * HALF:(h + 1) * HALF]


def assemble_body(y, occupation, *refs):
    both, lone = refs[8], refs[9:]
    for o in range(2):
        w = jnp.full((G, 128), occupation[2 * y[0] + o].astype(jnp.float32) * -0.5, jnp.float32)
        both[o, :, ROW:] = w
        lone[o][:, ROW:] = w
    for k in range(8):
        for o in range(2):
            for h in range(2):
                r = o * 12 + h * 6
                rows, lanes = slice(6 * k, 6 * k + 6), slice(h * HALF, (h + 1) * HALF)
                piece = refs[k][r:r + 6, :]
                both[o, rows, lanes] = piece
                lone[o][rows, lanes] = piece


def disperse_body(a, b, c0, c1, *outs):
    back = (c0, c1)
    for k in range(8):
        for o in range(2):
            for h in range(2):
                r = o * 12 + h * 6
                rows, lanes = slice(6 * k, 6 * k + 6), slice(h * HALF, (h + 1) * HALF)
                outs[k][r:r + 6, :] = a[o, rows, lanes] + b[o, rows, lanes] + back[o][rows, lanes]


def unpack_body(y, *refs):
    keep, give = refs[8:]
    flip = y[0] != 0
    for o in range(2):
        for h in range(2):
            r = o * 12 + h * 6
            total = refs[0][r:r + 6, :]
            for k in range(1, 8):
                total = total + refs[k][r:r + 6, :]
            for x in range(3):
                a, b = total[x:x + 1], total[x + 3:x + 4]
                keep[x, o:o + 1, h * HALF:(h + 1) * HALF] = jnp.where(flip, b, a)
                give[x, o:o + 1, h * HALF:(h + 1) * HALF] = jnp.where(flip, a, b)


def kernel(first, idx, own, twin, vis, ktab, fx, ix, fz, iz, *refs):
    prior = () if first else refs[:2]
    home, away, back, spec, *bufs = refs[len(prior):]
    gi, gj = idx[0], idx[1]
    once = idx[2] if first else idx[3]
    slots = 5 if first else 4

    def pick(i, lanes):
        return jnp.where(i < 2, own[i & 1, :, lanes], twin[i & 1, :, lanes])

    def ours(i, lanes):
        return own[i, :, lanes] if i < 2 else twin[i - 2, :, lanes]

    def enter_one(yb, rows, cols, zed):
        lanes = pl.ds(pl.multiple_of(yb * LB, LB), LB)
        for p in range(slots):
            r = ours(p, lanes) * vis[:, lanes] if p < 4 else pick(gi, lanes) * pick(gj, lanes)
            rows[p * G:(p + 1) * G, :] = apply(fx[...], r)
        for c in range(3):
            cols[c * 128:(c + 1) * 128, :] = rows[:, c * 128:(c + 1) * 128].T
        for y in range(YB):
            zed[y] = apply(fz[...], cols[y * G:(y + 1) * G, :])
        spec[:, pl.ds(pl.multiple_of(yb * YB, YB), YB), :] = jnp.swapaxes(zed[...], 0, 1)

    def enter(k, _):
        for u in range(6):
            enter_one(k * 6 + u, *bufs[u % 2 * 3:u % 2 * 3 + 3])
        return 0

    lax.fori_loop(0, G // YB // 6, enter, 0)

    def half_in(kz):
        return apply(fz[...], spec[kz]) * ktab[kz]

    for u in range(12):
        bufs[-1][u] = half_in(u)

    def middle(k, _):
        done = [apply(iz[...], bufs[-1][u]) for u in range(12)]
        for u in range(12):
            bufs[-1][u] = half_in((k + 1) * 12 + u)
        for u in range(12):
            spec[k * 12 + u] = done[u]
        return 0

    lax.fori_loop(0, G // 12 - 1, middle, 0)
    for u in range(12):
        spec[G - 12 + u] = apply(iz[...], bufs[-1][u])

    def spread(w):
        return jnp.concatenate([w] * (LB // 128), axis=1)

    keep = jnp.where(once != 0, 0.0, 1.0)
    tail = slice(ROW, WITH_W)
    wo = [spread((own if i < 2 else twin)[i % 2, 0:1, tail] * keep) for i in range(4)]
    wv = spread(vis[0:1, tail])
    if first:
        wj = spread(jnp.where(gj < 2, own[gj & 1, 0:1, tail], twin[gj & 1, 0:1, tail]))
        wg = jnp.where(gi < 2, wj, 0.0)
        wt = jnp.where(gi < 2, 0.0, wj)

    def leave_one(yb, rows, cols, zed):
        lanes = pl.ds(pl.multiple_of(yb * LB, LB), LB)
        zed[...] = jnp.swapaxes(spec[:, pl.ds(pl.multiple_of(yb * YB, YB), YB), :], 0, 1)
        for y in range(YB):
            cols[y * G:(y + 1) * G, :] = apply(iz[...], zed[y])
        for c in range(3):
            rows[:, c * 128:(c + 1) * 128] = cols[c * 128:(c + 1) * 128, :].T
        total = None
        v = vis[:, lanes] * wv
        for i in range(4):
            p = apply(ix[...], rows[i * G:(i + 1) * G, :])
            side = i // 2
            term = v * p
            if not first:
                term = term + prior[side][i % 2, :, lanes]
            (home, away)[side][i % 2, :, lanes] = term
            o = ours(i, lanes) * wo[i] * p
            total = o if total is None else total + o
        back[:, lanes] = total
        if first:
            p = pick(gj, lanes) * apply(ix[...], rows[4 * G:5 * G, :])
            home[gi & 1, :, lanes] = home[gi & 1, :, lanes] + p * wg
            away[gi & 1, :, lanes] = away[gi & 1, :, lanes] + p * wt

    def leave(k, _):
        for u in range(6):
            leave_one(k * 6 + u, *bufs[u % 2 * 3:u % 2 * 3 + 3])
        return 0

    lax.fori_loop(0, G // YB // 6, leave, 0)


def pair_solver(first, *args):
    return pl.pallas_call(
        functools.partial(kernel, first),
        out_shape=[f32(2, G, ROW), f32(2, G, ROW), f32(G, ROW)],
        in_specs=[SM] + [VM] * (len(args) - 1),
        out_specs=[VM] * 3,
        scratch_shapes=[
            pltpu.VMEM((G, G, WIDE), jnp.float32),
        ] + [
            pltpu.VMEM((WIDE, LB), jnp.float32),
            pltpu.VMEM((LB, WIDE), jnp.float32),
            pltpu.VMEM((YB, G, WIDE), jnp.float32),
        ] * 2 + [pltpu.VMEM((12, G, WIDE), jnp.float32)],
        compiler_params=pltpu.CompilerParams(vmem_limit_bytes=24 << 20),
        cost_estimate=pl.CostEstimate(flops=5 * 10**9, bytes_accessed=10**7, transcendentals=0),
    )(*args)


def stacked(m):
    top = lax.reduce_precision(m, 8, 7)
    hi = top.astype(jnp.bfloat16)
    lo = (m - top).astype(jnp.bfloat16)
    return jnp.concatenate([jnp.concatenate([hi, hi], 1), jnp.concatenate([lo, jnp.zeros_like(lo)], 1)], 0)


def plain_basis():
    k = np.arange(G)
    m = np.where(k <= G // 2, k, k - G // 2)
    ang = (2.0 * np.pi / G) * (m[:, None] * k[None, :] % G)
    return np.where((k <= G // 2)[:, None], np.cos(ang), np.sin(ang)).astype(np.float32)


def basis(place):
    k = jnp.arange(G, dtype=jnp.int32)
    m = jnp.where(k <= G // 2, k, k - G // 2)
    ang = (2.0 * np.pi / G) * ((m[:, None] * place[None, :]) % G).astype(jnp.float32)
    return jnp.where((k <= G // 2)[:, None], jnp.cos(ang), jnp.sin(ang))


def kernel_table(cutoff):
    def freq(shape, dim):
        k = lax.broadcasted_iota(jnp.int32, shape, dim) % G
        m = jnp.where(k <= G // 2, k, k - G // 2)
        return m * m, jnp.where((k == 0) | (k == G // 2), 1.0, 2.0)

    (a, wa), (b, wb), (c, wc) = freq((G, 1, 1), 0), freq((1, G, 1), 1), freq((1, 1, WIDE), 2)
    n = a + b + c
    ratios = n.astype(jnp.float32) * 0.5
    screen = jnp.where(n > 0, (1.0 - jnp.exp(-ratios)) / jnp.maximum(ratios, 0.5), 1.0)
    return jnp.where(n <= cutoff, 4.0 * screen * (wa * wb * wc / float(G**3)), 0.0)


def ring(block, axis, source):
    return lax.ppermute(block, axis, [(source(i), i) for i in range(lax.axis_size(axis))])


def partner(i):
    return (i + 8) % 16


def along(k):
    return lambda i: i // 8 * 8 + (i + k) % 8


def twin_of(i):
    return i ^ 1


OFFSETS = ((1, 0), (0, 1), (1, 1), (1, 3), (2, 1), (3, 2), None, (2, 0))
ORDER = ((2, 4, 6, 7, 0, 1, 3, 5), (0, 1, 3, 5, 2, 4, 6, 7))
MATCH = (5, 3, 2, 1, 4, 0, 6, 7)


def class_of(core, z, v):
    kind = ORDER[v][z]
    return MATCH[kind] if core else kind


def source_chip(kind, x, y):
    if kind == 6:
        px, py = x // 2, y // 2
        px, py = {(0, 0): (0, 1), (0, 1): (1, 0), (1, 0): (1, 1), (1, 1): (0, 0)}[(px, py)]
        return px * 2 + x % 2, py * 2 + y % 2
    dx, dy = OFFSETS[kind]
    return (x + dx) % 4, (y + dy) % 4


def visit_route(v, both_ways=True):
    pairs = []
    for b in range(16):
        for g in range(16):
            core, z = b % 2, g % 8
            kind = class_of(core, z, v)
            x, y = source_chip(kind, b // 2 % 4, g // 8 * 2 + b // 8)
            if both_ways or kind != 7:
                pairs.append(((((y % 2) * 4 + x) * 2 + core) * 16 + y // 2 * 8 + z, b * 16 + g))
    return pairs


def returned(back, v):
    return lax.ppermute(back, ("band", "grid"), [(d, s) for s, d in visit_route(v, False)])


def gather_blocks(b0):
    got = {0: b0}
    for k, source, hop in (
        (2, 0, 2), (6, 0, 6), (1, 0, 1), (7, 0, 7),
        (3, 2, 1), (5, 6, 7), (4, 2, 2),
    ):
        got[k] = ring(got[source], "grid", along(hop))
    return [got[k] for k in range(8)]


def scatter_blocks(part):
    return [part[0]] + [ring(part[k], "grid", along(-k)) for k in (4, 3, 5, 2, 6, 1, 7)]


def on_device(orbitals, occupation, cutoff):
    axes = ("band", "grid")
    g = lax.axis_index("grid")
    core = lax.axis_index("band") % 2
    z, y = g % 8, g // 8
    y1 = y.reshape(1)
    slab = orbitals.transpose(1, 0, 2)
    give = jnp.where(y == 0, slab[:, 2:], slab[:, :2])
    came = ring(give, "grid", partner)
    blk = small_call(pack_body, [f32(24, HALF)], y1, slab, came, scalars=1)

    got = gather_blocks(blk)
    e = z * 2 + core
    once = [z == ORDER[v].index(7) for v in range(2)]
    idx = jnp.stack([e // 4 ^ 2 * core, e % 4 ^ 2 * core] + [o.astype(jnp.int32) for o in once])
    r = jnp.arange(G, dtype=jnp.int32)
    turned = basis(3 * (r // 3 % 2 * 8 + (z + r // 6) % 8) + r % 3)
    plain = jnp.asarray(plain_basis())
    tables = (kernel_table(cutoff), stacked(turned), stacked(turned.T), stacked(plain), stacked(plain.T))
    got, idx, tables = lax.optimization_barrier((got, idx, tables))
    own, *lone = small_call(
        assemble_body, [f32(2, G, WITH_W), f32(G, WITH_W), f32(G, WITH_W)], y1, occupation, *got, scalars=2
    )
    vis0 = lax.ppermute(lone[0], axes, visit_route(0))
    twin = ring(own, "band", twin_of)
    held, vis0 = lax.optimization_barrier((lone[1], vis0))
    vis1 = lax.ppermute(held, axes, visit_route(1))

    home, away, back = pair_solver(True, idx, own, twin, vis0, *tables)
    ret0 = returned(back, 0)
    home, away, back = pair_solver(False, idx, own, twin, vis1, *tables, home, away)
    ret1 = returned(back, 1)
    swapped = ring(away, "band", twin_of)
    part = small_call(disperse_body, [f32(24, HALF)] * 8, home, swapped, ret0, ret1)
    keep, give = small_call(unpack_body, [f32(3, 2, ROW)] * 2, y1, *scatter_blocks(part), scalars=1)
    came = ring(give, "grid", partner)
    out = jnp.concatenate([jnp.where(y == 0, keep, came), jnp.where(y == 0, came, keep)], axis=1)
    return out.transpose(1, 0, 2)


def solution(mesh):
    placed = (P("band", "grid", None), P("band"), P())
    return jax.shard_map(
        on_device, mesh=mesh, in_specs=placed, out_specs=P("band", "grid", None), check_vma=False
    )
```

```python
import functools

import numpy as np
import jax
import jax.numpy as jnp
from jax import lax
from jax.experimental import pallas as pl
from jax.experimental.pallas import tpu as pltpu
from jax.sharding import PartitionSpec as P


G = 48
ROW = G * G
HALF = ROW // 2
WITH_W = ROW + 128
WIDE = 256
YB = 8
LB = YB * G
VM = pl.BlockSpec(memory_space=pltpu.VMEM)
SM = pl.BlockSpec(memory_space=pltpu.SMEM)


def split2(x):
    hi = x.astype(jnp.bfloat16)
    lo = (x - hi.astype(jnp.float32)).astype(jnp.bfloat16)
    return jnp.concatenate([hi, lo], axis=0)


def apply(mat, x):
    both = jnp.dot(mat, split2(x), preferred_element_type=jnp.float32)
    return both[:G] + both[G:]


def f32(*shape):
    return jax.ShapeDtypeStruct(shape, jnp.float32)


def small_call(body, outs, *args, scalars=0):
    many = len(outs) > 1
    return pl.pallas_call(
        body,
        out_shape=outs if many else outs[0],
        in_specs=[SM] * scalars + [VM] * (len(args) - scalars),
        out_specs=[VM] * len(outs) if many else VM,
        compiler_params=pltpu.CompilerParams(vmem_limit_bytes=8 << 20),
        cost_estimate=pl.CostEstimate(flops=10**6, bytes_accessed=10**6, transcendentals=0),
    )(*args)


def pack_body(y, slab, came, blk):
    flip = y[0] != 0
    for o in range(2):
        for x in range(3):
            mine = jnp.where(flip, slab[x, o + 2:o + 3, :], slab[x, o:o + 1, :])
            other = came[x, o:o + 1, :]
            a = jnp.where(flip, other, mine)
            b = jnp.where(flip, mine, other)
            for h in range(2):
                r = o * 12 + h * 6 + x
                blk[r:r + 1, :] = a[:, h * HALF:(h + 1) * HALF]
                blk[r + 3:r + 4, :] = b[:, h * HALF:(h + 1) * HALF]


def assemble_body(y, occupation, *refs):
    both, lone = refs[8], refs[9:]
    for o in range(2):
        w = jnp.full((G, 128), occupation[2 * y[0] + o].astype(jnp.float32) * -0.5, jnp.float32)
        both[o, :, ROW:] = w
        lone[o][:, ROW:] = w
    for k in range(8):
        for o in range(2):
            for h in range(2):
                r = o * 12 + h * 6
                rows, lanes = slice(6 * k, 6 * k + 6), slice(h * HALF, (h + 1) * HALF)
                piece = refs[k][r:r + 6, :]
                both[o, rows, lanes] = piece
                lone[o][rows, lanes] = piece


def disperse_body(a, b, c0, c1, *outs):
    back = (c0, c1)
    for k in range(8):
        for o in range(2):
            for h in range(2):
                r = o * 12 + h * 6
                rows, lanes = slice(6 * k, 6 * k + 6), slice(h * HALF, (h + 1) * HALF)
                outs[k][r:r + 6, :] = a[o, rows, lanes] + b[o, rows, lanes] + back[o][rows, lanes]


def unpack_body(y, *refs):
    keep, give = refs[8:]
    flip = y[0] != 0
    for o in range(2):
        for h in range(2):
            r = o * 12 + h * 6
            total = refs[0][r:r + 6, :]
            for k in range(1, 8):
                total = total + refs[k][r:r + 6, :]
            for x in range(3):
                a, b = total[x:x + 1], total[x + 3:x + 4]
                keep[x, o:o + 1, h * HALF:(h + 1) * HALF] = jnp.where(flip, b, a)
                give[x, o:o + 1, h * HALF:(h + 1) * HALF] = jnp.where(flip, a, b)


def kernel(first, idx, own, twin, vis, ktab, fx, ix, fz, iz, *refs):
    prior = () if first else refs[:2]
    home, away, back, spec, *bufs = refs[len(prior):]
    gi, gj = idx[0], idx[1]
    once = idx[2] if first else idx[3]
    slots = 5 if first else 4

    def pick(i, lanes):
        return jnp.where(i < 2, own[i & 1, :, lanes], twin[i & 1, :, lanes])

    def ours(i, lanes):
        return own[i, :, lanes] if i < 2 else twin[i - 2, :, lanes]

    def enter_one(yb, rows, cols, zed):
        lanes = pl.ds(pl.multiple_of(yb * LB, LB), LB)
        for p in range(slots):
            r = ours(p, lanes) * vis[:, lanes] if p < 4 else pick(gi, lanes) * pick(gj, lanes)
            rows[p * G:(p + 1) * G, :] = apply(fx[...], r)
        for c in range(3):
            cols[c * 128:(c + 1) * 128, :] = rows[:, c * 128:(c + 1) * 128].T
        for y in range(YB):
            zed[y] = apply(fz[...], cols[y * G:(y + 1) * G, :])
        spec[:, pl.ds(pl.multiple_of(yb * YB, YB), YB), :] = jnp.swapaxes(zed[...], 0, 1)

    def enter(k, _):
        for u in range(6):
            enter_one(k * 6 + u, *bufs[u % 2 * 3:u % 2 * 3 + 3])
        return 0

    lax.fori_loop(0, G // YB // 6, enter, 0)

    def half_in(kz):
        return apply(fz[...], spec[kz]) * ktab[kz]

    for u in range(12):
        bufs[-1][u] = half_in(u)

    def middle(k, _):
        done = [apply(iz[...], bufs[-1][u]) for u in range(12)]
        for u in range(12):
            bufs[-1][u] = half_in((k + 1) * 12 + u)
        for u in range(12):
            spec[k * 12 + u] = done[u]
        return 0

    lax.fori_loop(0, G // 12 - 1, middle, 0)
    for u in range(12):
        spec[G - 12 + u] = apply(iz[...], bufs[-1][u])

    def spread(w):
        return jnp.concatenate([w] * (LB // 128), axis=1)

    keep = jnp.where(once != 0, 0.0, 1.0)
    tail = slice(ROW, WITH_W)
    wo = [spread((own if i < 2 else twin)[i % 2, 0:1, tail] * keep) for i in range(4)]
    wv = spread(vis[0:1, tail])
    if first:
        wj = spread(jnp.where(gj < 2, own[gj & 1, 0:1, tail], twin[gj & 1, 0:1, tail]))
        wg = jnp.where(gi < 2, wj, 0.0)
        wt = jnp.where(gi < 2, 0.0, wj)

    def leave_one(yb, rows, cols, zed):
        lanes = pl.ds(pl.multiple_of(yb * LB, LB), LB)
        zed[...] = jnp.swapaxes(spec[:, pl.ds(pl.multiple_of(yb * YB, YB), YB), :], 0, 1)
        for y in range(YB):
            cols[y * G:(y + 1) * G, :] = apply(iz[...], zed[y])
        for c in range(3):
            rows[:, c * 128:(c + 1) * 128] = cols[c * 128:(c + 1) * 128, :].T
        total = None
        v = vis[:, lanes] * wv
        for i in range(4):
            p = apply(ix[...], rows[i * G:(i + 1) * G, :])
            side = i // 2
            term = v * p
            if not first:
                term = term + prior[side][i % 2, :, lanes]
            (home, away)[side][i % 2, :, lanes] = term
            o = ours(i, lanes) * wo[i] * p
            total = o if total is None else total + o
        back[:, lanes] = total
        if first:
            p = pick(gj, lanes) * apply(ix[...], rows[4 * G:5 * G, :])
            home[gi & 1, :, lanes] = home[gi & 1, :, lanes] + p * wg
            away[gi & 1, :, lanes] = away[gi & 1, :, lanes] + p * wt

    def leave(k, _):
        for u in range(6):
            leave_one(k * 6 + u, *bufs[u % 2 * 3:u % 2 * 3 + 3])
        return 0

    lax.fori_loop(0, G // YB // 6, leave, 0)


def pair_solver(first, *args):
    return pl.pallas_call(
        functools.partial(kernel, first),
        out_shape=[f32(2, G, ROW), f32(2, G, ROW), f32(G, ROW)],
        in_specs=[SM] + [VM] * (len(args) - 1),
        out_specs=[VM] * 3,
        scratch_shapes=[
            pltpu.VMEM((G, G, WIDE), jnp.float32),
        ] + [
            pltpu.VMEM((WIDE, LB), jnp.float32),
            pltpu.VMEM((LB, WIDE), jnp.float32),
            pltpu.VMEM((YB, G, WIDE), jnp.float32),
        ] * 2 + [pltpu.VMEM((12, G, WIDE), jnp.float32)],
        compiler_params=pltpu.CompilerParams(vmem_limit_bytes=24 << 20),
        cost_estimate=pl.CostEstimate(flops=5 * 10**9, bytes_accessed=10**7, transcendentals=0),
    )(*args)


def stacked(m):
    top = lax.reduce_precision(m, 8, 7)
    hi = top.astype(jnp.bfloat16)
    lo = (m - top).astype(jnp.bfloat16)
    return jnp.concatenate([jnp.concatenate([hi, hi], 1), jnp.concatenate([lo, jnp.zeros_like(lo)], 1)], 0)


def plain_basis():
    k = np.arange(G)
    m = np.where(k <= G // 2, k, k - G // 2)
    ang = (2.0 * np.pi / G) * (m[:, None] * k[None, :] % G)
    return np.where((k <= G // 2)[:, None], np.cos(ang), np.sin(ang)).astype(np.float32)


def basis(place):
    k = jnp.arange(G, dtype=jnp.int32)
    m = jnp.where(k <= G // 2, k, k - G // 2)
    ang = (2.0 * np.pi / G) * ((m[:, None] * place[None, :]) % G).astype(jnp.float32)
    return jnp.where((k <= G // 2)[:, None], jnp.cos(ang), jnp.sin(ang))


def kernel_table(cutoff):
    def freq(shape, dim):
        k = lax.broadcasted_iota(jnp.int32, shape, dim) % G
        m = jnp.where(k <= G // 2, k, k - G // 2)
        return m * m, jnp.where((k == 0) | (k == G // 2), 1.0, 2.0)

    (a, wa), (b, wb), (c, wc) = freq((G, 1, 1), 0), freq((1, G, 1), 1), freq((1, 1, WIDE), 2)
    n = a + b + c
    ratios = n.astype(jnp.float32) * 0.5
    screen = jnp.where(n > 0, (1.0 - jnp.exp(-ratios)) / jnp.maximum(ratios, 0.5), 1.0)
    return jnp.where(n <= cutoff, 4.0 * screen * (wa * wb * wc / float(G**3)), 0.0)


def ring(block, axis, source):
    return lax.ppermute(block, axis, [(source(i), i) for i in range(lax.axis_size(axis))])


def partner(i):
    return (i + 8) % 16


def along(k):
    return lambda i: i // 8 * 8 + (i + k) % 8


def twin_of(i):
    return i ^ 1


OFFSETS = ((1, 0), (0, 1), (1, 1), (1, 3), (2, 1), (3, 2), None, (2, 0))
ORDER = ((2, 4, 6, 7, 0, 1, 3, 5), (0, 1, 3, 5, 2, 4, 6, 7))
MATCH = (5, 3, 2, 1, 4, 0, 6, 7)


def class_of(core, z, v):
    kind = ORDER[v][z]
    return MATCH[kind] if core else kind


def source_chip(kind, x, y):
    if kind == 6:
        px, py = x // 2, y // 2
        px, py = {(0, 0): (0, 1), (0, 1): (1, 0), (1, 0): (1, 1), (1, 1): (0, 0)}[(px, py)]
        return px * 2 + x % 2, py * 2 + y % 2
    dx, dy = OFFSETS[kind]
    return (x + dx) % 4, (y + dy) % 4


def visit_route(v, both_ways=True):
    pairs = []
    for b in range(16):
        for g in range(16):
            core, z = b % 2, g % 8
            kind = class_of(core, z, v)
            x, y = source_chip(kind, b // 2 % 4, g // 8 * 2 + b // 8)
            if both_ways or kind != 7:
                pairs.append(((((y % 2) * 4 + x) * 2 + core) * 16 + y // 2 * 8 + z, b * 16 + g))
    return pairs


def returned(back, v):
    return lax.ppermute(back, ("band", "grid"), [(d, s) for s, d in visit_route(v, False)])


def gather_blocks(b0):
    got = {0: b0}
    for k, source, hop in (
        (2, 0, 2), (6, 0, 6), (1, 0, 1), (7, 0, 7), (3, 2, 1), (4, 2, 2), (5, 6, 7),
    ):
        got[k] = ring(got[source], "grid", along(hop))
    return [got[k] for k in range(8)]


def scatter_blocks(part):
    came = [part[0]]
    for k in (3, 5, 4, 2, 6, 1, 7):
        came.append(ring(part[k], "grid", along(-k)))
    return came


def on_device(orbitals, occupation, cutoff):
    axes = ("band", "grid")
    g = lax.axis_index("grid")
    core = lax.axis_index("band") % 2
    z, y = g % 8, g // 8
    y1 = y.reshape(1)
    slab = orbitals.transpose(1, 0, 2)
    give = jnp.where(y == 0, slab[:, 2:], slab[:, :2])
    came = ring(give, "grid", partner)
    blk = small_call(pack_body, [f32(24, HALF)], y1, slab, came, scalars=1)

    got = gather_blocks(blk)
    e = z * 2 + core
    once = [z == ORDER[v].index(7) for v in range(2)]
    idx = jnp.stack([e // 4 ^ 2 * core, e % 4 ^ 2 * core] + [o.astype(jnp.int32) for o in once])
    r = jnp.arange(G, dtype=jnp.int32)
    turned = basis(3 * (r // 3 % 2 * 8 + (z + r // 6) % 8) + r % 3)
    plain = jnp.asarray(plain_basis())
    tables = (kernel_table(cutoff), stacked(turned), stacked(turned.T), stacked(plain), stacked(plain.T))
    got, idx, tables = lax.optimization_barrier((got, idx, tables))
    own, *lone = small_call(
        assemble_body, [f32(2, G, WITH_W), f32(G, WITH_W), f32(G, WITH_W)], y1, occupation, *got, scalars=2
    )
    vis0 = lax.ppermute(lone[0], axes, visit_route(0))
    twin = ring(own, "band", twin_of)
    held, vis0 = lax.optimization_barrier((lone[1], vis0))
    vis1 = lax.ppermute(held, axes, visit_route(1))

    home, away, back = pair_solver(True, idx, own, twin, vis0, *tables)
    ret0 = returned(back, 0)
    home, away, back = pair_solver(False, idx, own, twin, vis1, *tables, home, away)
    ret1 = returned(back, 1)
    swapped = ring(away, "band", twin_of)
    part = small_call(disperse_body, [f32(24, HALF)] * 8, home, swapped, ret0, ret1)
    keep, give = small_call(unpack_body, [f32(3, 2, ROW)] * 2, y1, *scatter_blocks(part), scalars=1)
    came = ring(give, "grid", partner)
    out = jnp.concatenate([jnp.where(y == 0, keep, came), jnp.where(y == 0, came, keep)], axis=1)
    return out.transpose(1, 0, 2)


def solution(mesh):
    placed = (P("band", "grid", None), P("band"), P())
    return jax.shard_map(
        on_device, mesh=mesh, in_specs=placed, out_specs=P("band", "grid", None), check_vma=False
    )
```

```python
import functools

import numpy as np
import jax
import jax.numpy as jnp
from jax import lax
from jax.experimental import pallas as pl
from jax.experimental.pallas import tpu as pltpu
from jax.sharding import PartitionSpec as P


G = 48
ROW = G * G
HALF = ROW // 2
WITH_W = ROW + 128
WIDE = 256
YB = 8
LB = YB * G
VM = pl.BlockSpec(memory_space=pltpu.VMEM)
SM = pl.BlockSpec(memory_space=pltpu.SMEM)


def split2(x):
    hi = x.astype(jnp.bfloat16)
    lo = (x - hi.astype(jnp.float32)).astype(jnp.bfloat16)
    return jnp.concatenate([hi, lo], axis=0)


def apply(mat, x):
    both = jnp.dot(mat, split2(x), preferred_element_type=jnp.float32)
    return both[:G] + both[G:]


def f32(*shape):
    return jax.ShapeDtypeStruct(shape, jnp.float32)


def small_call(body, outs, *args, scalars=0):
    many = len(outs) > 1
    return pl.pallas_call(
        body,
        out_shape=outs if many else outs[0],
        in_specs=[SM] * scalars + [VM] * (len(args) - scalars),
        out_specs=[VM] * len(outs) if many else VM,
        compiler_params=pltpu.CompilerParams(vmem_limit_bytes=8 << 20),
        cost_estimate=pl.CostEstimate(flops=10**6, bytes_accessed=10**6, transcendentals=0),
    )(*args)


def pack_body(y, slab, came, blk):
    flip = y[0] != 0
    for o in range(2):
        for x in range(3):
            mine = jnp.where(flip, slab[x, o + 2:o + 3, :], slab[x, o:o + 1, :])
            other = came[x, o:o + 1, :]
            a = jnp.where(flip, other, mine)
            b = jnp.where(flip, mine, other)
            for h in range(2):
                r = o * 12 + h * 6 + x
                blk[r:r + 1, :] = a[:, h * HALF:(h + 1) * HALF]
                blk[r + 3:r + 4, :] = b[:, h * HALF:(h + 1) * HALF]


def assemble_body(y, occupation, *refs):
    both, lone = refs[8], refs[9:]
    for o in range(2):
        w = jnp.full((G, 128), occupation[2 * y[0] + o].astype(jnp.float32) * -0.5, jnp.float32)
        both[o, :, ROW:] = w
        lone[o][:, ROW:] = w
    for k in range(8):
        for o in range(2):
            for h in range(2):
                r = o * 12 + h * 6
                rows, lanes = slice(6 * k, 6 * k + 6), slice(h * HALF, (h + 1) * HALF)
                piece = refs[k][r:r + 6, :]
                both[o, rows, lanes] = piece
                lone[o][rows, lanes] = piece


def disperse_body(a, b, c0, c1, *outs):
    back = (c0, c1)
    for k in range(8):
        for o in range(2):
            for h in range(2):
                r = o * 12 + h * 6
                rows, lanes = slice(6 * k, 6 * k + 6), slice(h * HALF, (h + 1) * HALF)
                outs[k][r:r + 6, :] = a[o, rows, lanes] + b[o, rows, lanes] + back[o][rows, lanes]


def unpack_body(y, *refs):
    keep, give = refs[8:]
    flip = y[0] != 0
    for o in range(2):
        for h in range(2):
            r = o * 12 + h * 6
            total = refs[0][r:r + 6, :]
            for k in range(1, 8):
                total = total + refs[k][r:r + 6, :]
            for x in range(3):
                a, b = total[x:x + 1], total[x + 3:x + 4]
                keep[x, o:o + 1, h * HALF:(h + 1) * HALF] = jnp.where(flip, b, a)
                give[x, o:o + 1, h * HALF:(h + 1) * HALF] = jnp.where(flip, a, b)


def kernel(first, idx, own, twin, vis, ktab, fx, ix, fz, iz, *refs):
    prior = () if first else refs[:2]
    home, away, back, spec, *bufs = refs[len(prior):]
    gi, gj = idx[0], idx[1]
    once = idx[2] if first else idx[3]
    slots = 5 if first else 4

    def pick(i, lanes):
        return jnp.where(i < 2, own[i & 1, :, lanes], twin[i & 1, :, lanes])

    def ours(i, lanes):
        return own[i, :, lanes] if i < 2 else twin[i - 2, :, lanes]

    def enter_one(yb, rows, cols, zed):
        lanes = pl.ds(pl.multiple_of(yb * LB, LB), LB)
        for p in range(slots):
            r = ours(p, lanes) * vis[:, lanes] if p < 4 else pick(gi, lanes) * pick(gj, lanes)
            rows[p * G:(p + 1) * G, :] = apply(fx[...], r)
        for c in range(3):
            cols[c * 128:(c + 1) * 128, :] = rows[:, c * 128:(c + 1) * 128].T
        for y in range(YB):
            zed[y] = apply(fz[...], cols[y * G:(y + 1) * G, :])
        spec[:, pl.ds(pl.multiple_of(yb * YB, YB), YB), :] = jnp.swapaxes(zed[...], 0, 1)

    def enter(k, _):
        for u in range(6):
            enter_one(k * 6 + u, *bufs[u % 2 * 3:u % 2 * 3 + 3])
        return 0

    lax.fori_loop(0, G // YB // 6, enter, 0)

    def half_in(kz):
        return apply(fz[...], spec[kz]) * ktab[kz]

    for u in range(16):
        bufs[-1][u] = half_in(u)

    def middle(k, _):
        done = [apply(iz[...], bufs[-1][u]) for u in range(16)]
        for u in range(16):
            bufs[-1][u] = half_in((k + 1) * 16 + u)
        for u in range(16):
            spec[k * 16 + u] = done[u]
        return 0

    lax.fori_loop(0, G // 16 - 1, middle, 0)
    for u in range(16):
        spec[G - 16 + u] = apply(iz[...], bufs[-1][u])

    def spread(w):
        return jnp.concatenate([w] * (LB // 128), axis=1)

    keep = jnp.where(once != 0, 0.0, 1.0)
    tail = slice(ROW, WITH_W)
    wo = [spread((own if i < 2 else twin)[i % 2, 0:1, tail] * keep) for i in range(4)]
    wv = spread(vis[0:1, tail])
    if first:
        wj = spread(jnp.where(gj < 2, own[gj & 1, 0:1, tail], twin[gj & 1, 0:1, tail]))
        wg = jnp.where(gi < 2, wj, 0.0)
        wt = jnp.where(gi < 2, 0.0, wj)

    def leave_one(yb, rows, cols, zed):
        lanes = pl.ds(pl.multiple_of(yb * LB, LB), LB)
        zed[...] = jnp.swapaxes(spec[:, pl.ds(pl.multiple_of(yb * YB, YB), YB), :], 0, 1)
        for y in range(YB):
            cols[y * G:(y + 1) * G, :] = apply(iz[...], zed[y])
        for c in range(3):
            rows[:, c * 128:(c + 1) * 128] = cols[c * 128:(c + 1) * 128, :].T
        total = None
        v = vis[:, lanes] * wv
        for i in range(4):
            p = apply(ix[...], rows[i * G:(i + 1) * G, :])
            side = i // 2
            term = v * p
            if not first:
                term = term + prior[side][i % 2, :, lanes]
            (home, away)[side][i % 2, :, lanes] = term
            o = ours(i, lanes) * wo[i] * p
            total = o if total is None else total + o
        back[:, lanes] = total
        if first:
            p = pick(gj, lanes) * apply(ix[...], rows[4 * G:5 * G, :])
            home[gi & 1, :, lanes] = home[gi & 1, :, lanes] + p * wg
            away[gi & 1, :, lanes] = away[gi & 1, :, lanes] + p * wt

    def leave(k, _):
        for u in range(6):
            leave_one(k * 6 + u, *bufs[u % 2 * 3:u % 2 * 3 + 3])
        return 0

    lax.fori_loop(0, G // YB // 6, leave, 0)


def pair_solver(first, *args):
    return pl.pallas_call(
        functools.partial(kernel, first),
        out_shape=[f32(2, G, ROW), f32(2, G, ROW), f32(G, ROW)],
        in_specs=[SM] + [VM] * (len(args) - 1),
        out_specs=[VM] * 3,
        scratch_shapes=[
            pltpu.VMEM((G, G, WIDE), jnp.float32),
        ] + [
            pltpu.VMEM((WIDE, LB), jnp.float32),
            pltpu.VMEM((LB, WIDE), jnp.float32),
            pltpu.VMEM((YB, G, WIDE), jnp.float32),
        ] * 2 + [pltpu.VMEM((16, G, WIDE), jnp.float32)],
        compiler_params=pltpu.CompilerParams(vmem_limit_bytes=24 << 20),
        cost_estimate=pl.CostEstimate(flops=5 * 10**9, bytes_accessed=10**7, transcendentals=0),
    )(*args)


def stacked(m):
    top = lax.reduce_precision(m, 8, 7)
    hi = top.astype(jnp.bfloat16)
    lo = (m - top).astype(jnp.bfloat16)
    return jnp.concatenate([jnp.concatenate([hi, hi], 1), jnp.concatenate([lo, jnp.zeros_like(lo)], 1)], 0)


def plain_basis():
    k = np.arange(G)
    m = np.where(k <= G // 2, k, k - G // 2)
    ang = (2.0 * np.pi / G) * (m[:, None] * k[None, :] % G)
    return np.where((k <= G // 2)[:, None], np.cos(ang), np.sin(ang)).astype(np.float32)


def basis(place):
    k = jnp.arange(G, dtype=jnp.int32)
    m = jnp.where(k <= G // 2, k, k - G // 2)
    ang = (2.0 * np.pi / G) * ((m[:, None] * place[None, :]) % G).astype(jnp.float32)
    return jnp.where((k <= G // 2)[:, None], jnp.cos(ang), jnp.sin(ang))


def kernel_table(cutoff):
    def freq(shape, dim):
        k = lax.broadcasted_iota(jnp.int32, shape, dim) % G
        m = jnp.where(k <= G // 2, k, k - G // 2)
        return m * m, jnp.where((k == 0) | (k == G // 2), 1.0, 2.0)

    (a, wa), (b, wb), (c, wc) = freq((G, 1, 1), 0), freq((1, G, 1), 1), freq((1, 1, WIDE), 2)
    n = a + b + c
    ratios = n.astype(jnp.float32) * 0.5
    screen = jnp.where(n > 0, (1.0 - jnp.exp(-ratios)) / jnp.maximum(ratios, 0.5), 1.0)
    return jnp.where(n <= cutoff, 4.0 * screen * (wa * wb * wc / float(G**3)), 0.0)


def ring(block, axis, source):
    return lax.ppermute(block, axis, [(source(i), i) for i in range(lax.axis_size(axis))])


def partner(i):
    return (i + 8) % 16


def along(k):
    return lambda i: i // 8 * 8 + (i + k) % 8


def twin_of(i):
    return i ^ 1


OFFSETS = ((1, 0), (0, 1), (1, 1), (1, 3), (2, 1), (3, 2), None, (2, 0))
ORDER = ((2, 4, 6, 7, 0, 1, 3, 5), (0, 1, 3, 5, 2, 4, 6, 7))
MATCH = (5, 3, 2, 1, 4, 0, 6, 7)


def class_of(core, z, v):
    kind = ORDER[v][z]
    return MATCH[kind] if core else kind


def source_chip(kind, x, y):
    if kind == 6:
        px, py = x // 2, y // 2
        px, py = {(0, 0): (0, 1), (0, 1): (1, 0), (1, 0): (1, 1), (1, 1): (0, 0)}[(px, py)]
        return px * 2 + x % 2, py * 2 + y % 2
    dx, dy = OFFSETS[kind]
    return (x + dx) % 4, (y + dy) % 4


def visit_route(v, both_ways=True):
    pairs = []
    for b in range(16):
        for g in range(16):
            core, z = b % 2, g % 8
            kind = class_of(core, z, v)
            x, y = source_chip(kind, b // 2 % 4, g // 8 * 2 + b // 8)
            if both_ways or kind != 7:
                pairs.append(((((y % 2) * 4 + x) * 2 + core) * 16 + y // 2 * 8 + z, b * 16 + g))
    return pairs


def returned(back, v):
    return lax.ppermute(back, ("band", "grid"), [(d, s) for s, d in visit_route(v, False)])


def gather_blocks(b0):
    got = {0: b0}
    for k, source, hop in (
        (2, 0, 2), (6, 0, 6), (1, 0, 1), (7, 0, 7), (3, 2, 1), (4, 2, 2), (5, 6, 7),
    ):
        got[k] = ring(got[source], "grid", along(hop))
    return [got[k] for k in range(8)]


def scatter_blocks(part):
    came = [part[0]]
    for k in (3, 5, 4, 2, 6, 1, 7):
        came.append(ring(part[k], "grid", along(-k)))
    return came


def on_device(orbitals, occupation, cutoff):
    axes = ("band", "grid")
    g = lax.axis_index("grid")
    core = lax.axis_index("band") % 2
    z, y = g % 8, g // 8
    y1 = y.reshape(1)
    slab = orbitals.transpose(1, 0, 2)
    give = jnp.where(y == 0, slab[:, 2:], slab[:, :2])
    came = ring(give, "grid", partner)
    blk = small_call(pack_body, [f32(24, HALF)], y1, slab, came, scalars=1)

    got = gather_blocks(blk)
    e = z * 2 + core
    once = [z == ORDER[v].index(7) for v in range(2)]
    idx = jnp.stack([e // 4 ^ 2 * core, e % 4 ^ 2 * core] + [o.astype(jnp.int32) for o in once])
    r = jnp.arange(G, dtype=jnp.int32)
    turned = basis(3 * (r // 3 % 2 * 8 + (z + r // 6) % 8) + r % 3)
    plain = jnp.asarray(plain_basis())
    tables = (kernel_table(cutoff), stacked(turned), stacked(turned.T), stacked(plain), stacked(plain.T))
    got, idx, tables = lax.optimization_barrier((got, idx, tables))
    own, *lone = small_call(
        assemble_body, [f32(2, G, WITH_W), f32(G, WITH_W), f32(G, WITH_W)], y1, occupation, *got, scalars=2
    )
    vis0 = lax.ppermute(lone[0], axes, visit_route(0))
    twin = ring(own, "band", twin_of)
    held, vis0 = lax.optimization_barrier((lone[1], vis0))
    vis1 = lax.ppermute(held, axes, visit_route(1))

    home, away, back = pair_solver(True, idx, own, twin, vis0, *tables)
    ret0 = returned(back, 0)
    home, away, back = pair_solver(False, idx, own, twin, vis1, *tables, home, away)
    ret1 = returned(back, 1)
    swapped = ring(away, "band", twin_of)
    part = small_call(disperse_body, [f32(24, HALF)] * 8, home, swapped, ret0, ret1)
    keep, give = small_call(unpack_body, [f32(3, 2, ROW)] * 2, y1, *scatter_blocks(part), scalars=1)
    came = ring(give, "grid", partner)
    out = jnp.concatenate([jnp.where(y == 0, keep, came), jnp.where(y == 0, came, keep)], axis=1)
    return out.transpose(1, 0, 2)


def solution(mesh):
    placed = (P("band", "grid", None), P("band"), P())
    return jax.shard_map(
        on_device, mesh=mesh, in_specs=placed, out_specs=P("band", "grid", None), check_vma=False
    )
```
